256 devices in a mesh: ra: 16 (over x_hi, y, core), dec: 16 (over z, x_lo).
Axes of the slice: x: 4 (x_hi: 2, x_lo: 2; x = x_hi * 2 + x_lo), y: 4, z: 8, core: 2. Of those that a mesh axis runs over, the one named last changes fastest.
Arguments:
- design: float32 [5, 80, 64, 4096], P(None, None, 'ra', 'dec'), may hold values from -6 to 6
- observed: float32 [80, 64, 4096], P(None, 'ra', 'dec'), may hold values from -6 to 6
- weight: float32 [80, 64, 4096], P(None, 'ra', 'dec'), may hold values from 0.3 to 3
- params: float32 [5, 64, 4096], P(None, 'ra', 'dec'), may hold values from -4 to 4
- offsets: int32 [80, 64, 4096], P(None, 'ra', 'dec'), may hold values from 0 to 8, as said below
- counts: int32 [64, 4096], P('ra', 'dec'), may hold values from 10 to 80, as said below
Outputs:
- new_params: float32 [5, 64, 4096], P(None, 'ra', 'dec')
- reduced_chi: float32 [], replicated
The draws below stay inside these ranges and needn't reach their ends.
Inputs may be any that keep to these rules, and one draw needn't show every extreme that they name: `offsets`: in the first and the last latitude row of cells no offset steps outside the grid in latitude. `counts`: cells near the middle latitude hold more live observations; the two middle latitude rows hold 80.
All inputs are finite; a program needn't handle non-finite values.
Results may differ from the reference program's by a relative error of at most 0.0003.
Values sent between devices are 32-bit elements; how exact they have to be, the bound alone decides.
No kernel may reach another device: no remote copies, remote signals or barrier semaphores. Data moves between devices by JAX's collectives and lax.ppermute only.
A program may use at most 64 MiB of HBM per device.

```python
import math
import jax
import jax.numpy as jnp
from jax import lax

NPAR = 5
OBS = 80
NX = 64
NY = 4096


def draw_offsets(key, part):
    key_ra, key_dec = jax.random.split(key)
    step_ra = jax.random.randint(key_ra, (OBS, NX, NY), -1, 2)
    step_dec = jax.random.randint(key_dec, (OBS, NX, NY), -1, 2)
    row = lax.broadcasted_iota(jnp.int32, (OBS, NX, NY), 2)
    step_dec = jnp.where((row == 0) & (step_dec < 0), 0, step_dec)
    step_dec = jnp.where((row == NY - 1) & (step_dec > 0), 0, step_dec)
    return ((step_ra + 1) * 3 + step_dec + 1).astype(jnp.int32)


def draw_counts(key, part):
    lowest = max(1, OBS // 8)
    row = lax.broadcasted_iota(jnp.int32, (NX, NY), 1)
    distance = jnp.abs(2 * row + 1 - NY)
    highest = OBS - (OBS - lowest) * distance // NY
    drawn = jax.random.randint(key, (NX, NY), lowest, highest + 1)
    return jnp.where(distance <= 1, OBS, drawn).astype(jnp.int32)


def levels(key, extent, shards, smallest, largest):
    loudness = 1.0
    for dim, parts in shards:
        draws = jax.random.uniform(jax.random.fold_in(jax.random.fold_in(key, 6), dim), (parts,), jnp.float32, smallest / len(shards), largest / len(shards))
        loudness = loudness * jnp.repeat(jnp.exp(draws), extent[dim] // parts).reshape((-1,) + (1,) * (len(extent) - 1 - dim))
    return loudness


def bell_draw(rng, shape, width, bound, cuts=(), kind=jnp.bfloat16):
    values = jax.random.normal(rng, shape, jnp.float32) * width
    if len(cuts) > 0:
        values = levels(rng, shape, cuts, -0.22, 0.18) * values
    return jnp.clip(values, min=-bound, max=bound).astype(kind)


def setup_inputs(seed: int = 0) -> dict:
    arg_keys = jax.random.split(jax.random.key(seed), 7)
    return {
        "design": bell_draw(arg_keys[0], (NPAR, OBS, NX, NY), 1.0, 6.0, ((2, 16), (3, 16)), jnp.float32),
        "observed": bell_draw(arg_keys[1], (OBS, NX, NY), 1.0, 6.0, ((1, 16), (2, 16)), jnp.float32),
        "weight": jnp.clip(jnp.exp(math.log(3.0) - 2.3025851 * jax.random.uniform(arg_keys[2], (OBS, NX, NY), jnp.float32) ** levels(arg_keys[2], (OBS, NX, NY), ((1, 16), (2, 16)), -0.2, 0.2)), 0.3, 3.0),
        "params": bell_draw(arg_keys[3], (NPAR, NX, NY), 0.5, 4.0, ((1, 16), (2, 16)), jnp.float32),
        "offsets": draw_offsets(jax.random.fold_in(arg_keys[6], 71), 0),
        "counts": draw_counts(jax.random.fold_in(arg_keys[6], 71), 0),
    }


def pair_list():
    pairs = []
    for first in range(5):
        for second in range(first, 5):
            pairs.append((first, second))
    return pairs

def contributions(design, observed, masked_weight, source_params):
    resid = observed
    for comp in range(5):
        resid = resid - design[comp] * source_params[comp][None]
    weighted = masked_weight * resid
    rows = []
    for comp in range(5):
        rows.append(lax.optimization_barrier(jnp.sum(design[comp] * weighted, axis=0)))
    for first, second in pair_list():
        rows.append(lax.optimization_barrier(jnp.sum(masked_weight * design[first] * design[second], axis=0)))
    return (jnp.stack(rows, axis=0), jnp.sum(weighted * resid))

def solve_blocks(stacked):
    rhs = [stacked[comp] for comp in range(5)]
    normal = [[None] * 5 for item in range(5)]
    for place, pair in enumerate(pair_list()):
        first, second = pair
        value = stacked[5 + place]
        if first == second:
            value = value + 1.0
        normal[first][second] = value
        normal[second][first] = value
    lower = [[None] * 5 for item in range(5)]
    for first in range(5):
        for second in range(first + 1):
            running = normal[first][second]
            for inner in range(second):
                running = running - lower[first][inner] * lower[second][inner]
            if first == second:
                lower[first][first] = jnp.sqrt(running)
            else:
                lower[first][second] = running / lower[second][second]
    forward = []
    for first in range(5):
        running = rhs[first]
        for inner in range(first):
            running = running - lower[first][inner] * forward[inner]
        forward.append(running / lower[first][first])
    answer = [None] * 5
    for first in range(4, -1, -1):
        running = forward[first]
        for inner in range(first + 1, 5):
            running = running - lower[inner][first] * answer[inner]
        answer[first] = running / lower[first][first]
    return jnp.stack(answer, axis=0)

def reference(design, observed, weight, params, offsets, counts):
    slots = lax.broadcasted_iota(jnp.int32, observed.shape, 0)
    live = slots < counts[None]
    total = jnp.zeros((20,) + params.shape[1:], jnp.float32)
    chi = jnp.zeros((), jnp.float32)
    for code in range(9):
        step_ra = code // 3 - 1
        step_dec = code % 3 - 1
        source_params = jnp.roll(params, (-step_ra, -step_dec), axis=(1, 2))
        masked_weight = jnp.where(live & (offsets == code), weight, jnp.zeros_like(weight))
        terms, chi_part = contributions(design, observed, masked_weight, source_params)
        total = total + jnp.roll(terms, (step_ra, step_dec), axis=(1, 2))
        chi = chi + chi_part
    new_params = params + solve_blocks(total)
    reduced_chi = chi / jnp.sum(counts).astype(jnp.float32)
    return (new_params, reduced_chi)
```

```python
import jax
import jax.numpy as jnp
from jax import lax
from jax.experimental import pallas as pl
from jax.experimental.pallas import tpu as pltpu
from jax.sharding import Mesh
from jax.sharding import PartitionSpec as P

RA = ("ra_0", "ra_1", "ra_2")
DEC = ("dec_0", "dec_1")
ALL = RA + DEC

PAIRS = [(p, q) for p in range(5) for q in range(p, 5)]
NQ = 20
VM = pl.BlockSpec(memory_space=pltpu.VMEM)
SM = pl.BlockSpec(memory_space=pltpu.SMEM)
BLOCK = (8, 128)


def blocked(x):
    lead = x.shape[:-2]
    x = x.reshape(lead + (4, 2, 128))
    x = jnp.swapaxes(x, -3, -2)
    return x.reshape(lead + BLOCK)


def unblocked(x):
    lead = x.shape[:-2]
    x = x.reshape(lead + (2, 4, 128))
    x = jnp.swapaxes(x, -3, -2)
    return x.reshape(lead + (4, 256))


def grids():
    lane = lax.broadcasted_iota(jnp.int32, BLOCK, 1)
    sub = lax.broadcasted_iota(jnp.int32, BLOCK, 0)
    return lane, sub & 3, sub >> 2


def lanes(x, by):
    by = by % 128
    return x if by == 0 else pltpu.roll(x, by, 1)


def subs(x, by):
    by = by % 8
    return x if by == 0 else pltpu.roll(x, by, 0)


def edge_kernel(params_ref, out_ref):
    lane, row, half = grids()
    out = jnp.zeros(BLOCK, jnp.float32)
    for p in range(5):
        value = params_ref[p]
        out = jnp.where(lane == p, jnp.where(half == 0, lanes(value, p), lanes(value, p + 1)), out)
    out_ref[...] = out


def column_pack(minus, plus, q, out, lane, half):
    return jnp.where(lane == q, jnp.where(half == 0, lanes(minus, q), lanes(plus, q + 1)), out)


def shift_sum(minus, mid, plus, lane, half):
    down = lanes(minus, 127)
    down = jnp.where(lane == 127, jnp.where(half == 0, subs(down, 4), 0.0), down)
    up = lanes(plus, 1)
    up = jnp.where(lane == 0, jnp.where(half == 1, subs(up, 4), 0.0), up)
    return mid + down + up


def sums_kernel(design_ref, observed_ref, weight_ref, offsets_ref, counts_ref, total_ref, edges_ref, acc_ref):
    lane, row, half = grids()
    counts = counts_ref[...]
    for code in range(9):

        def body(k, acc, code=code):
            hit = (offsets_ref[k] == code) & (counts > k)
            w = jnp.where(hit, weight_ref[k], 0.0)
            d = [design_ref[p, k] for p in range(5)]
            o = observed_ref[k]
            wd = [w * x for x in d]
            new = [wd[p] * o for p in range(5)] + [wd[p] * d[q] for p, q in PAIRS]
            return tuple(a + b for a, b in zip(acc, new))

        acc = lax.fori_loop(0, 80, body, (jnp.zeros(BLOCK, jnp.float32),) * NQ, unroll=4)
        for q in range(NQ):
            acc_ref[code, q] = acc[q]
    inner = jnp.zeros(BLOCK, jnp.float32)
    outer = jnp.zeros(BLOCK, jnp.float32)
    low = [jnp.zeros(BLOCK, jnp.float32) for _ in range(5)]
    high = [jnp.zeros(BLOCK, jnp.float32) for _ in range(5)]
    for q in range(NQ):
        stay = []
        leave = []
        for b in range(3):
            back, same, ahead = acc_ref[b, q], acc_ref[3 + b, q], acc_ref[6 + b, q]
            stay.append(
                same + jnp.where(row < 3, subs(back, 7), 0.0) + jnp.where(row > 0, subs(ahead, 1), 0.0)
            )
            leave.append(jnp.where(row == 0, back, jnp.where(row == 3, ahead, 0.0)))
        total_ref[q] = shift_sum(*stay, lane, half)
        inner = column_pack(stay[0], stay[2], q, inner, lane, half)
        outer = column_pack(leave[0], leave[2], q, outer, lane, half)
        out = shift_sum(*leave, lane, half)
        g, i = divmod(q, 4)
        low[g] = jnp.where(row == i, subs(out, i), low[g])
        high[g] = jnp.where(row == i, subs(out, i - 3), high[g])
    for g in range(5):
        edges_ref[g] = low[g]
        edges_ref[5 + g] = high[g]
    edges_ref[10] = outer
    total_ref[NQ] = inner


def message_kernel(params_ref, edges_ref, dec_a_ref, dec_b_ref, to_a_ref, to_b_ref, halo_ref):
    lane, row, half = grids()
    dec_odd = lax.axis_index("dec_1")
    ra_odd = lax.axis_index("ra_2")
    halo = jnp.where((half == 0) == (dec_odd == 0), dec_a_ref[...], dec_b_ref[...])
    halo_ref[...] = halo
    low = [edges_ref[g] for g in range(5)] + [jnp.zeros(BLOCK, jnp.float32) for _ in range(2)]
    high = [edges_ref[5 + g] for g in range(5)] + [jnp.zeros(BLOCK, jnp.float32) for _ in range(2)]
    for p in range(5):
        g, i = divmod(NQ + p, 4)
        value = params_ref[p]
        low[g] = jnp.where(row == i, subs(value, i), low[g])
        high[g] = jnp.where(row == i, subs(value, i - 3), high[g])
    for g in range(7):
        to_a_ref[g] = jnp.where(ra_odd == 0, high[g], low[g])
        to_b_ref[g] = jnp.where(ra_odd == 0, low[g], high[g])
    for ref in (to_a_ref, to_b_ref):
        ref[7] = edges_ref[10]
        ref[8] = halo


def chi_kernel(
    design_ref, observed_ref, weight_ref, offsets_ref, counts_ref, params_ref,
    total_ref, from_a_ref, from_b_ref, halo_ref, total_out_ref, send_ref, win_ref,
):
    lane, row, half = grids()
    ra_odd = lax.axis_index("ra_2")
    dec = lax.axis_index(DEC)
    me = lax.axis_index(RA) * 16 + dec

    def from_low(g):
        return jnp.where(ra_odd == 0, from_b_ref[g], from_a_ref[g])

    def from_high(g):
        return jnp.where(ra_odd == 0, from_a_ref[g], from_b_ref[g])

    halo = halo_ref[...]
    around = [
        jnp.where(row == 0, subs(from_low(8), 5), subs(halo, 1)),
        halo,
        jnp.where(row == 3, subs(from_high(8), 3), subs(halo, 7)),
    ]
    around = [subs(x, 4) for x in around]
    for p in range(5):
        g, i = divmod(NQ + p, 4)
        value = params_ref[p]
        shifted = [
            jnp.where(row == 0, subs(from_low(g), -i), subs(value, 1)),
            value,
            jnp.where(row == 3, subs(from_high(g), 3 - i), subs(value, 7)),
        ]
        for a in range(3):
            x = shifted[a]
            y = lanes(x, 1)
            y = jnp.where(lane == 0, jnp.where(half == 1, subs(y, 4), lanes(around[a], -p)), y)
            win_ref[3 * a, p] = y
            win_ref[3 * a + 1, p] = x
            y = lanes(x, 127)
            y = jnp.where(lane == 127, jnp.where(half == 0, subs(y, 4), lanes(around[a], 127 - p)), y)
            win_ref[3 * a + 2, p] = y

    counts = counts_ref[...]

    def body(k, acc):
        code = offsets_ref[k]
        hits = [code == c for c in range(1, 9)]
        resid = observed_ref[k]
        for p in range(5):
            source = win_ref[0, p]
            for c in range(1, 9):
                source = jnp.where(hits[c - 1], win_ref[c, p], source)
            resid = resid - design_ref[p, k] * source
        w = jnp.where(counts > k, weight_ref[k], 0.0)
        return acc + w * resid * resid

    chi = jnp.sum(lax.fori_loop(0, 80, body, jnp.zeros(BLOCK, jnp.float32), unroll=4))
    count = jnp.sum(counts.astype(jnp.float32))

    for q in range(NQ):
        g, i = divmod(q, 4)
        total_out_ref[q] = (
            total_ref[q]
            + jnp.where(row == 0, subs(from_low(g), -i), 0.0)
            + jnp.where(row == 3, subs(from_high(g), 3 - i), 0.0)
        )
    column = (
        total_ref[NQ]
        + jnp.where(row == 0, subs(from_low(7), 5), 0.0)
        + jnp.where(row == 3, subs(from_high(7), 3), 0.0)
    )
    column = jnp.where(lane < NQ, column, 0.0)
    flat = column
    for r in range(1, 4):
        flat = jnp.where(row == r, lanes(column, 32 * r), flat)
    down = jnp.sum(jnp.where(half == 0, flat, 0.0), axis=0, keepdims=True)
    up = jnp.sum(jnp.where(half == 1, flat, 0.0), axis=0, keepdims=True)
    base = jnp.where(lane == NQ, chi, jnp.where(lane == NQ + 1, count, 0.0))
    for g in range(32):
        send_ref[pl.ds(8 * g, 8), :] = base

    @pl.when(dec > 0)
    def _():
        send_ref[pl.ds(me - 1, 1), :] = base[:1] + down

    @pl.when(dec < 15)
    def _():
        send_ref[pl.ds(me + 1, 1), :] = base[:1] + up


def solve(rhs, normal):
    lower = [[None] * 5 for _ in range(5)]
    inverse = [None] * 5
    for first in range(5):
        for second in range(first + 1):
            running = normal[second][first]
            for inner in range(second):
                running = running - lower[first][inner] * lower[second][inner]
            if first == second:
                inverse[first] = 1.0 / jnp.sqrt(running)
            else:
                lower[first][second] = running * inverse[second]
    forward = []
    for first in range(5):
        running = rhs[first]
        for inner in range(first):
            running = running - lower[first][inner] * forward[inner]
        forward.append(running * inverse[first])
    answer = [None] * 5
    for first in range(4, -1, -1):
        running = forward[first]
        for inner in range(first + 1, 5):
            running = running - lower[inner][first] * answer[inner]
        answer[first] = running * inverse[first]
    return answer


def solve_kernel(params_ref, total_ref, got_ref, new_ref, chi_ref):
    lane, row, half = grids()
    me = lax.axis_index(ALL)

    def column(source):
        line = jnp.broadcast_to(got_ref[pl.ds(source, 1), :], BLOCK)
        out = line
        for r in range(1, 4):
            out = jnp.where(row == r, lanes(line, -32 * r), out)
        return out

    from_low = column(jnp.maximum(me - 1, 0))
    from_high = column(jnp.minimum(me + 1, 255))
    sums = []
    for q in range(NQ):
        sums.append(
            total_ref[q]
            + jnp.where((lane == 0) & (half == 0), lanes(from_low, -q), 0.0)
            + jnp.where((lane == 127) & (half == 1), lanes(from_high, 127 - q), 0.0)
        )
    normal = [[None] * 5 for _ in range(5)]
    for place, (p, q) in enumerate(PAIRS):
        normal[p][q] = sums[5 + place]
        normal[q][p] = sums[5 + place]
    params = [params_ref[p] for p in range(5)]
    rhs = []
    for p in range(5):
        running = sums[p]
        for q in range(5):
            running = running - normal[p][q] * params[q]
        rhs.append(running)
    for p in range(5):
        normal[p][p] = normal[p][p] + 1.0
    delta = solve(rhs, normal)
    for p in range(5):
        new_ref[p] = params[p] + delta[p]
    all_sums = got_ref[pl.ds(0, 8), :]
    for g in range(1, 32):
        all_sums = all_sums + got_ref[pl.ds(8 * g, 8), :]
    chi = jnp.sum(jnp.where(lane == NQ, all_sums, 0.0))
    count = jnp.sum(jnp.where(lane == NQ + 1, all_sums, 0.0))
    chi_ref[0, 0] = chi / count


def exchange(value, axes, pairs):
    both = [(i, j) for i, j in pairs] + [(j, i) for i, j in pairs]
    return lax.ppermute(value, axes, both)


def f32(*shape):
    return jax.ShapeDtypeStruct(shape, jnp.float32)


def call(kernel, outs, n_in, scratch=(), flops=1000, smem_last=False):
    specs = [VM] * len(outs)
    if smem_last:
        specs[-1] = SM
    return pl.pallas_call(
        kernel,
        out_shape=tuple(outs),
        in_specs=[VM] * n_in,
        out_specs=tuple(specs),
        scratch_shapes=list(scratch),
        cost_estimate=pl.CostEstimate(flops=flops, bytes_accessed=100000, transcendentals=0),
    )


def per_device(design, observed, weight, params, offsets, counts):
    design, observed, weight, params, offsets, counts = (
        blocked(x) for x in (design, observed, weight, params, offsets, counts)
    )
    (edge,) = call(edge_kernel, [f32(*BLOCK)], 1)(params)
    dec_b = exchange(edge, DEC, [(i, i + 1) for i in range(1, 15, 2)])
    dec_a = exchange(edge, DEC, [(i, i + 1) for i in range(0, 16, 2)])
    total, edges = call(
        sums_kernel, [f32(NQ + 1, *BLOCK), f32(11, *BLOCK)], 5,
        [pltpu.VMEM((9, NQ) + BLOCK, jnp.float32)], 30_000_000,
    )(design, observed, weight, offsets, counts)
    to_a, to_b, halo = call(message_kernel, [f32(9, *BLOCK), f32(9, *BLOCK), f32(*BLOCK)], 4)(
        params, edges, dec_a, dec_b
    )
    from_b = exchange(to_b, RA, [(i, (i + 1) % 16) for i in range(1, 16, 2)])
    from_a = exchange(to_a, RA, [(i, i + 1) for i in range(0, 16, 2)])
    total, send = call(
        chi_kernel, [f32(NQ, *BLOCK), f32(256, 128)], 10,
        [pltpu.VMEM((9, 5) + BLOCK, jnp.float32)], 5_000_000,
    )(design, observed, weight, offsets, counts, params, total, from_a, from_b, halo)
    got = lax.all_to_all(send.reshape(256, 1, 128), ALL, 0, 0, tiled=True).reshape(256, 128)
    new, chi = call(solve_kernel, [f32(5, *BLOCK), f32(1, 1)], 3, (), 100000, True)(params, total, got)
    return unblocked(new), chi.reshape(())


def solution(mesh):
    finer = Mesh(mesh.devices.reshape(2, 4, 2, 8, 2), ALL)
    return jax.shard_map(
        per_device,
        mesh=finer,
        in_specs=(
            P(None, None, RA, DEC),
            P(None, RA, DEC),
            P(None, RA, DEC),
            P(None, RA, DEC),
            P(None, RA, DEC),
            P(RA, DEC),
        ),
        out_specs=(P(None, RA, DEC), P()),
        check_vma=False,
    )
```

```python
import jax
import jax.numpy as jnp
from jax import lax
from jax.experimental import pallas as pl
from jax.experimental.pallas import tpu as pltpu
from jax.sharding import Mesh
from jax.sharding import PartitionSpec as P

RA = ("ra_0", "ra_1", "ra_2")
DEC = ("dec_0", "dec_1")
ALL = RA + DEC

PAIRS = [(p, q) for p in range(5) for q in range(p, 5)]
NQ = 20
EDGE_FLOPS = 20_000_000_000
VM = pl.BlockSpec(memory_space=pltpu.VMEM)
SM = pl.BlockSpec(memory_space=pltpu.SMEM)
BLOCK = (8, 128)


def blocked(x):
    lead = x.shape[:-2]
    x = x.reshape(lead + (4, 2, 128))
    x = jnp.swapaxes(x, -3, -2)
    return x.reshape(lead + BLOCK)


def unblocked(x):
    lead = x.shape[:-2]
    x = x.reshape(lead + (2, 4, 128))
    x = jnp.swapaxes(x, -3, -2)
    return x.reshape(lead + (4, 256))


def grids():
    lane = lax.broadcasted_iota(jnp.int32, BLOCK, 1)
    sub = lax.broadcasted_iota(jnp.int32, BLOCK, 0)
    return lane, sub & 3, sub >> 2


def lanes(x, by):
    by = by % 128
    return x if by == 0 else pltpu.roll(x, by, 1)


def subs(x, by):
    by = by % 8
    return x if by == 0 else pltpu.roll(x, by, 0)


def edge_kernel(params_ref, out_ref):
    lane, row, half = grids()
    out = jnp.zeros(BLOCK, jnp.float32)
    for p in range(5):
        value = params_ref[p]
        out = jnp.where(lane == p, jnp.where(half == 0, lanes(value, p), lanes(value, p + 1)), out)
    out_ref[...] = out


def column_pack(minus, plus, q, out, lane, half):
    return jnp.where(lane == q, jnp.where(half == 0, lanes(minus, q), lanes(plus, q + 1)), out)


def shift_sum(minus, mid, plus, lane, half):
    down = lanes(minus, 127)
    down = jnp.where(lane == 127, jnp.where(half == 0, subs(down, 4), 0.0), down)
    up = lanes(plus, 1)
    up = jnp.where(lane == 0, jnp.where(half == 1, subs(up, 4), 0.0), up)
    return mid + down + up


def accumulate(design_ref, observed_ref, weight_ref, code_ref, wanted):
    def body(k, acc):
        w = jnp.where(code_ref[k] == wanted, weight_ref[k], 0.0)
        d = [design_ref[p, k] for p in range(5)]
        o = observed_ref[k]
        wd = [w * x for x in d]
        new = [wd[p] * o for p in range(5)] + [wd[p] * d[q] for p, q in PAIRS]
        return tuple(x + y for x, y in zip(acc, new))

    return lax.fori_loop(0, 80, body, (jnp.zeros(BLOCK, jnp.float32),) * NQ, unroll=4)


def edge_code(b, row):
    return jnp.where(row == 0, b, jnp.where(row == 3, 6 + b, -1))


def leave_kernel(
    design_ref, observed_ref, weight_ref, offsets_ref, counts_ref, params_ref,
    to_a_ref, to_b_ref, code_ref, acc_ref,
):
    lane, row, half = grids()
    counts = counts_ref[...]
    ra_odd = lax.axis_index("ra_2")

    def mark(k, carry):
        code_ref[k] = jnp.where(counts > k, offsets_ref[k], 9)
        return carry

    lax.fori_loop(0, 80, mark, 0, unroll=8)
    for b in range(3):
        acc = accumulate(design_ref, observed_ref, weight_ref, code_ref, edge_code(b, row))
        for q in range(NQ):
            acc_ref[b, q] = acc[q]
    outer = jnp.zeros(BLOCK, jnp.float32)
    low = [jnp.zeros(BLOCK, jnp.float32) for _ in range(7)]
    high = [jnp.zeros(BLOCK, jnp.float32) for _ in range(7)]
    for q in range(NQ + 5):
        if q < NQ:
            leave = [acc_ref[b, q] for b in range(3)]
            outer = column_pack(leave[0], leave[2], q, outer, lane, half)
            value = shift_sum(*leave, lane, half)
        else:
            value = params_ref[q - NQ]
        g, i = divmod(q, 4)
        low[g] = jnp.where(row == i, subs(value, i), low[g])
        high[g] = jnp.where(row == i, subs(value, i - 3), high[g])
    for g in range(7):
        to_a_ref[g] = jnp.where(ra_odd == 0, high[g], low[g])
        to_b_ref[g] = jnp.where(ra_odd == 0, low[g], high[g])
    for ref in (to_a_ref, to_b_ref):
        ref[7] = outer
        ref[8] = jnp.zeros(BLOCK, jnp.float32)


def halo_kernel(dec_a_ref, dec_b_ref, in_a_ref, in_b_ref, to_a_ref, to_b_ref, halo_ref):
    lane, row, half = grids()
    dec_odd = lax.axis_index("dec_1")
    halo = jnp.where((half == 0) == (dec_odd == 0), dec_a_ref[...], dec_b_ref[...])
    halo_ref[...] = halo
    for g in range(8):
        to_a_ref[g] = in_a_ref[g]
        to_b_ref[g] = in_b_ref[g]
    to_a_ref[8] = halo
    to_b_ref[8] = halo


def columns_around(x, beyond, p, lane, half):
    below = lanes(x, 1)
    below = jnp.where(lane == 0, jnp.where(half == 1, subs(below, 4), lanes(beyond, -p)), below)
    above = lanes(x, 127)
    above = jnp.where(lane == 127, jnp.where(half == 0, subs(above, 4), lanes(beyond, 127 - p)), above)
    return below, x, above


def stay_kernel(
    design_ref, observed_ref, weight_ref, code_ref, params_ref, halo_ref,
    total_ref, acc_ref, win_ref,
):
    lane, row, half = grids()
    halo = subs(halo_ref[...], 4)
    for p in range(5):
        value = params_ref[p]
        for a in range(3):
            shift = (1, 0, 7)[a]
            found = columns_around(subs(value, shift), subs(halo, shift), p, lane, half)
            for b in range(3):
                win_ref[3 * a + b, p] = found[b]

    least = jnp.where(row == 0, 3, 0)
    most = jnp.where(row == 3, 5, 8)

    def body(k, acc):
        code = code_ref[k]
        hits = [code == c for c in range(1, 9)]
        resid = observed_ref[k]
        for p in range(5):
            source = win_ref[0, p]
            for c in range(1, 9):
                source = jnp.where(hits[c - 1], win_ref[c, p], source)
            resid = resid - design_ref[p, k] * source
        inside = (code >= least) & (code <= most)
        w = jnp.where(inside, weight_ref[k], 0.0)
        return acc + w * resid * resid

    total_ref[NQ + 1] = lax.fori_loop(0, 80, body, jnp.zeros(BLOCK, jnp.float32), unroll=4)
    for code in range(9):
        acc = accumulate(design_ref, observed_ref, weight_ref, code_ref, code)
        for q in range(NQ):
            acc_ref[code, q] = acc[q]
    inner = jnp.zeros(BLOCK, jnp.float32)
    for q in range(NQ):
        stay = []
        for b in range(3):
            back, same, ahead = acc_ref[b, q], acc_ref[3 + b, q], acc_ref[6 + b, q]
            stay.append(
                same + jnp.where(row < 3, subs(back, 7), 0.0) + jnp.where(row > 0, subs(ahead, 1), 0.0)
            )
        total_ref[q] = shift_sum(*stay, lane, half)
        inner = column_pack(stay[0], stay[2], q, inner, lane, half)
    total_ref[NQ] = inner


def chi_kernel(
    design_ref, observed_ref, weight_ref, code_ref, counts_ref,
    total_ref, from_a_ref, from_b_ref, total_out_ref, send_ref, win_ref,
):
    lane, row, half = grids()
    ra_odd = lax.axis_index("ra_2")
    dec = lax.axis_index(DEC)
    me = lax.axis_index(RA) * 16 + dec

    def from_low(g):
        return jnp.where(ra_odd == 0, from_b_ref[g], from_a_ref[g])

    def from_high(g):
        return jnp.where(ra_odd == 0, from_a_ref[g], from_b_ref[g])

    beyond = subs(jnp.where(row == 0, subs(from_low(8), 5), subs(from_high(8), 3)), 4)
    for p in range(5):
        g, i = divmod(NQ + p, 4)
        value = jnp.where(row == 0, subs(from_low(g), -i), subs(from_high(g), 3 - i))
        found = columns_around(value, beyond, p, lane, half)
        for b in range(3):
            win_ref[b, p] = found[b]

    wanted = [edge_code(b, row) for b in range(3)]

    def body(k, acc):
        code = code_ref[k]
        hits = [code == x for x in wanted]
        resid = observed_ref[k]
        for p in range(5):
            source = jnp.where(hits[1], win_ref[1, p], win_ref[0, p])
            source = jnp.where(hits[2], win_ref[2, p], source)
            resid = resid - design_ref[p, k] * source
        outside = hits[0] | hits[1] | hits[2]
        w = jnp.where(outside, weight_ref[k], 0.0)
        return acc + w * resid * resid

    chi = jnp.sum(lax.fori_loop(0, 80, body, total_ref[NQ + 1], unroll=4))
    count = jnp.sum(counts_ref[...].astype(jnp.float32))

    for q in range(NQ):
        g, i = divmod(q, 4)
        total_out_ref[q] = (
            total_ref[q]
            + jnp.where(row == 0, subs(from_low(g), -i), 0.0)
            + jnp.where(row == 3, subs(from_high(g), 3 - i), 0.0)
        )
    column = (
        total_ref[NQ]
        + jnp.where(row == 0, subs(from_low(7), 5), 0.0)
        + jnp.where(row == 3, subs(from_high(7), 3), 0.0)
    )
    column = jnp.where(lane < NQ, column, 0.0)
    flat = column
    for r in range(1, 4):
        flat = jnp.where(row == r, lanes(column, 32 * r), flat)
    down = jnp.sum(jnp.where(half == 0, flat, 0.0), axis=0, keepdims=True)
    up = jnp.sum(jnp.where(half == 1, flat, 0.0), axis=0, keepdims=True)
    base = jnp.where(lane == NQ, chi, jnp.where(lane == NQ + 1, count, 0.0))
    for g in range(32):
        send_ref[pl.ds(8 * g, 8), :] = base

    @pl.when(dec > 0)
    def _():
        send_ref[pl.ds(me - 1, 1), :] = base[:1] + down

    @pl.when(dec < 15)
    def _():
        send_ref[pl.ds(me + 1, 1), :] = base[:1] + up


def solve(rhs, normal):
    lower = [[None] * 5 for _ in range(5)]
    inverse = [None] * 5
    for first in range(5):
        for second in range(first + 1):
            running = normal[second][first]
            for inner in range(second):
                running = running - lower[first][inner] * lower[second][inner]
            if first == second:
                inverse[first] = 1.0 / jnp.sqrt(running)
            else:
                lower[first][second] = running * inverse[second]
    forward = []
    for first in range(5):
        running = rhs[first]
        for inner in range(first):
            running = running - lower[first][inner] * forward[inner]
        forward.append(running * inverse[first])
    answer = [None] * 5
    for first in range(4, -1, -1):
        running = forward[first]
        for inner in range(first + 1, 5):
            running = running - lower[inner][first] * answer[inner]
        answer[first] = running * inverse[first]
    return answer


def solve_kernel(params_ref, total_ref, got_ref, new_ref, chi_ref):
    lane, row, half = grids()
    me = lax.axis_index(ALL)

    def column(source):
        line = jnp.broadcast_to(got_ref[pl.ds(source, 1), :], BLOCK)
        out = line
        for r in range(1, 4):
            out = jnp.where(row == r, lanes(line, -32 * r), out)
        return out

    from_low = column(jnp.maximum(me - 1, 0))
    from_high = column(jnp.minimum(me + 1, 255))
    sums = []
    for q in range(NQ):
        sums.append(
            total_ref[q]
            + jnp.where((lane == 0) & (half == 0), lanes(from_low, -q), 0.0)
            + jnp.where((lane == 127) & (half == 1), lanes(from_high, 127 - q), 0.0)
        )
    normal = [[None] * 5 for _ in range(5)]
    for place, (p, q) in enumerate(PAIRS):
        normal[p][q] = sums[5 + place]
        normal[q][p] = sums[5 + place]
    params = [params_ref[p] for p in range(5)]
    rhs = []
    for p in range(5):
        running = sums[p]
        for q in range(5):
            running = running - normal[p][q] * params[q]
        rhs.append(running)
    for p in range(5):
        normal[p][p] = normal[p][p] + 1.0
    delta = solve(rhs, normal)
    for p in range(5):
        new_ref[p] = params[p] + delta[p]
    all_sums = got_ref[pl.ds(0, 8), :]
    for g in range(1, 32):
        all_sums = all_sums + got_ref[pl.ds(8 * g, 8), :]
    chi = jnp.sum(jnp.where(lane == NQ, all_sums, 0.0))
    count = jnp.sum(jnp.where(lane == NQ + 1, all_sums, 0.0))
    chi_ref[0, 0] = chi / count


def exchange(value, axes, pairs):
    both = [(i, j) for i, j in pairs] + [(j, i) for i, j in pairs]
    return lax.ppermute(value, axes, both)


def f32(*shape):
    return jax.ShapeDtypeStruct(shape, jnp.float32)


def call(kernel, outs, n_in, scratch=(), flops=1000, smem_last=False, mib=2):
    specs = [VM] * len(outs)
    if smem_last:
        specs[-1] = SM
    return pl.pallas_call(
        kernel,
        out_shape=tuple(outs),
        in_specs=[VM] * n_in,
        out_specs=tuple(specs),
        scratch_shapes=list(scratch),
        cost_estimate=pl.CostEstimate(flops=flops, bytes_accessed=100000, transcendentals=0),
        compiler_params=pltpu.CompilerParams(vmem_limit_bytes=mib << 20),
    )


def scratch(*shape):
    return pltpu.VMEM(shape + BLOCK, jnp.float32)


def per_device(design, observed, weight, params, offsets, counts):
    design, observed, weight, params, offsets, counts = (
        blocked(x) for x in (design, observed, weight, params, offsets, counts)
    )
    (edge,) = call(edge_kernel, [f32(*BLOCK)], 1, (), EDGE_FLOPS)(params)
    dec_b = exchange(edge, DEC, [(i, i + 1) for i in range(1, 15, 2)])
    dec_a = exchange(edge, DEC, [(i, i + 1) for i in range(0, 16, 2)])
    message = f32(9, *BLOCK)
    to_a, to_b, code = call(
        leave_kernel, [message, message, jax.ShapeDtypeStruct((80,) + BLOCK, jnp.int32)], 6,
        [scratch(3, NQ)], 10_000_000, mib=6,
    )(design, observed, weight, offsets, counts, params)
    slots = (design, observed, weight, code)
    to_a, to_b, halo = call(halo_kernel, [message, message, f32(*BLOCK)], 4)(dec_a, dec_b, to_a, to_b)
    from_b = exchange(to_b, RA, [(i, (i + 1) % 16) for i in range(1, 16, 2)])
    from_a = exchange(to_a, RA, [(i, i + 1) for i in range(0, 16, 2)])
    (total,) = call(
        stay_kernel, [f32(NQ + 2, *BLOCK)], 6, [scratch(9, NQ), scratch(9, 5)], 30_000_000, mib=6
    )(*slots, params, halo)
    total, send = call(
        chi_kernel, [f32(NQ, *BLOCK), f32(256, 128)], 8, [scratch(3, 5)], 5_000_000, mib=6
    )(*slots, counts, total, from_a, from_b)
    got = lax.all_to_all(send.reshape(256, 1, 128), ALL, 0, 0, tiled=True).reshape(256, 128)
    new, chi = call(solve_kernel, [f32(5, *BLOCK), f32(1, 1)], 3, (), 100000, True)(params, total, got)
    return unblocked(new), chi.reshape(())


def solution(mesh):
    finer = Mesh(mesh.devices.reshape(2, 4, 2, 8, 2), ALL)
    return jax.shard_map(
        per_device,
        mesh=finer,
        in_specs=(
            P(None, None, RA, DEC),
            P(None, RA, DEC),
            P(None, RA, DEC),
            P(None, RA, DEC),
            P(None, RA, DEC),
            P(RA, DEC),
        ),
        out_specs=(P(None, RA, DEC), P()),
        check_vma=False,
    )
```

```python
import jax
import jax.numpy as jnp
from jax import lax
from jax.experimental import pallas as pl
from jax.experimental.pallas import tpu as pltpu
from jax.sharding import Mesh
from jax.sharding import PartitionSpec as P

RA = ("ra_0", "ra_1", "ra_2")
DEC = ("dec_0", "dec_1")
ALL = RA + DEC

PAIRS = [(p, q) for p in range(5) for q in range(p, 5)]
NQ = 20
EDGE_FLOPS = 20_000_000_000
VM = pl.BlockSpec(memory_space=pltpu.VMEM)
SM = pl.BlockSpec(memory_space=pltpu.SMEM)
BLOCK = (8, 128)


def blocked(x):
    lead = x.shape[:-2]
    x = x.reshape(lead + (4, 2, 128))
    x = jnp.swapaxes(x, -3, -2)
    return x.reshape(lead + BLOCK)


def unblocked(x):
    lead = x.shape[:-2]
    x = x.reshape(lead + (2, 4, 128))
    x = jnp.swapaxes(x, -3, -2)
    return x.reshape(lead + (4, 256))


def grids():
    lane = lax.broadcasted_iota(jnp.int32, BLOCK, 1)
    sub = lax.broadcasted_iota(jnp.int32, BLOCK, 0)
    return lane, sub & 3, sub >> 2


def lanes(x, by):
    by = by % 128
    return x if by == 0 else pltpu.roll(x, by, 1)


def subs(x, by):
    by = by % 8
    return x if by == 0 else pltpu.roll(x, by, 0)


def edge_kernel(params_ref, out_ref):
    lane, _, half = grids()
    out = jnp.zeros(BLOCK, jnp.float32)
    for p in range(5):
        value = params_ref[p]
        out = jnp.where(lane == p, jnp.where(half == 0, lanes(value, p), lanes(value, p + 1)), out)
    out_ref[...] = out


def shift_sum(minus, mid, plus, lane, half):
    down = lanes(minus, 127)
    down = jnp.where(lane == 127, jnp.where(half == 0, subs(down, 4), 0.0), down)
    up = lanes(plus, 1)
    up = jnp.where(lane == 0, jnp.where(half == 1, subs(up, 4), 0.0), up)
    return mid + down + up


def accumulate(design_ref, observed_ref, weight_ref, code_ref, wanted):
    def body(k, acc):
        w = jnp.where(code_ref[k] == wanted, weight_ref[k], 0.0)
        d = [design_ref[p, k] for p in range(5)]
        o = observed_ref[k]
        wd = [w * x for x in d]
        new = [wd[p] * o for p in range(5)] + [wd[p] * d[q] for p, q in PAIRS]
        return tuple(x + y for x, y in zip(acc, new))

    return lax.fori_loop(0, 80, body, (jnp.zeros(BLOCK, jnp.float32),) * NQ, unroll=4)


def edge_code(b, row):
    return jnp.where(row == 0, b, jnp.where(row == 3, 6 + b, -1))


def by_neighbour(to_a_ref, to_b_ref, low, high, start=0):
    ra_odd = lax.axis_index("ra_2")
    for g in range(len(low)):
        to_a_ref[start + g] = jnp.where(ra_odd == 0, high[g], low[g])
        to_b_ref[start + g] = jnp.where(ra_odd == 0, low[g], high[g])


def pack_rows(values, row):
    count = (len(values) + 3) // 4
    low = [jnp.zeros(BLOCK, jnp.float32) for _ in range(count)]
    high = [jnp.zeros(BLOCK, jnp.float32) for _ in range(count)]
    for q, value in enumerate(values):
        g, i = divmod(q, 4)
        low[g] = jnp.where(row == i, subs(value, i), low[g])
        high[g] = jnp.where(row == i, subs(value, i - 3), high[g])
    return low, high


def column_kernel(
    design_ref, observed_ref, weight_ref, offsets_ref, counts_ref, params_ref, edge_ref,
    to_a_ref, to_b_ref, packed_ref, codes_ref, again_ref,
):
    lane, row, half = grids()
    again_ref[...] = edge_ref[...]
    packed = [jnp.zeros(BLOCK, jnp.float32) for _ in range(7)]
    codes = jnp.full(BLOCK, 9, jnp.int32)
    counts = jnp.zeros(BLOCK, jnp.int32)
    for k in range(80):
        here = lane == jnp.where(half == 0, k, (k + 127) % 128)
        values = [design_ref[p, k] for p in range(5)] + [observed_ref[k], weight_ref[k]]
        packed = [jnp.where(here, lanes(x, k), y) for x, y in zip(values, packed)]
        codes = jnp.where(here, lanes(offsets_ref[k], k), codes)
    counts = counts_ref[...]
    counts = jnp.where(half == 0, counts[:, :1], counts[:, 127:])
    slot = jnp.where(half == 0, lane, (lane + 1) & 127)
    codes = jnp.where(counts > slot, codes, 9)
    for i in range(7):
        packed_ref[i] = packed[i]
    codes_ref[...] = codes
    corner = edge_code(2 * half, row)
    outside = packed[:6] + [jnp.where(codes == corner, packed[6], 0.0)]
    low, high = pack_rows([params_ref[p] for p in range(5)], row)
    by_neighbour(to_a_ref, to_b_ref, low + outside, high + outside)


def flatten(x, row, half):
    flat = x
    for r in range(1, 4):
        flat = jnp.where(row == r, lanes(x, 32 * r), flat)
    return [jnp.sum(jnp.where(half == j, flat, 0.0), axis=0, keepdims=True) for j in range(2)]


def columns_around(x, beyond, p, lane, half):
    below = lanes(x, 1)
    below = jnp.where(lane == 0, jnp.where(half == 1, subs(below, 4), lanes(beyond, -p)), below)
    above = lanes(x, 127)
    above = jnp.where(lane == 127, jnp.where(half == 0, subs(above, 4), lanes(beyond, 127 - p)), above)
    return below, x, above


def inside_kernel(
    design_ref, observed_ref, weight_ref, offsets_ref, counts_ref, params_ref,
    packed_ref, codes_ref, dec_a_ref, dec_b_ref,
    lines_ref, chi_ref, halo_ref, code_ref, win_ref,
):
    lane, row, half = grids()
    zero = jnp.zeros(BLOCK, jnp.float32)
    d, o, weight, codes = [packed_ref[p] for p in range(5)], packed_ref[5], packed_ref[6], codes_ref[...]
    found = []
    for a in range(3):
        w = jnp.where(codes == 3 * a + 2 * half, weight, 0.0)
        wd = [w * x for x in d]
        terms = [wd[p] * o for p in range(5)] + [wd[p] * d[q] for p, q in PAIRS]
        out = zero
        for q in range(NQ):
            out = jnp.where(lane == q, jnp.sum(terms[q], axis=1, keepdims=True), out)
        found.append(out)
    back, same, ahead = found
    mid = same + jnp.where(row < 3, subs(back, 7), 0.0) + jnp.where(row > 0, subs(ahead, 1), 0.0)
    low = jnp.where(row == 3, subs(back, 3), 0.0)
    high = jnp.where(row == 0, subs(ahead, 5), 0.0)
    lines_ref[...] = jnp.zeros(BLOCK, jnp.float32)
    for i, x in enumerate((low, mid, high)):
        for j, line in enumerate(flatten(x, row, half)):
            lines_ref[2 * i + j : 2 * i + j + 1, :] = line
    counts = counts_ref[...]
    lines_ref[6:7, :] = jnp.where(lane[:1] == NQ + 1, jnp.sum(counts.astype(jnp.float32)), 0.0)

    dec_odd = lax.axis_index("dec_1")
    halo = jnp.where((half == 0) == (dec_odd == 0), dec_a_ref[...], dec_b_ref[...])
    halo = subs(halo, 4)
    halo_ref[...] = halo
    for p in range(5):
        value = params_ref[p]
        for a in range(3):
            shift = (1, 0, 7)[a]
            found = columns_around(subs(value, shift), subs(halo, shift), p, lane, half)
            for b in range(3):
                win_ref[3 * a + b, p] = found[b]

    least = jnp.where(row == 0, 3, 0)
    most = jnp.where(row == 3, 5, 8)

    def body(k, acc):
        code = jnp.where(counts > k, offsets_ref[k], 9)
        code_ref[k] = code
        hits = [code == c for c in range(1, 9)]
        resid = observed_ref[k]
        for p in range(5):
            source = win_ref[0, p]
            for c in range(1, 9):
                source = jnp.where(hits[c - 1], win_ref[c, p], source)
            resid = resid - design_ref[p, k] * source
        inside = (code >= least) & (code <= most)
        w = jnp.where(inside, weight_ref[k], 0.0)
        return acc + w * resid * resid

    chi_ref[...] = lax.fori_loop(0, 80, body, zero, unroll=4)


def ra_sides(from_a_ref, from_b_ref):
    ra_odd = lax.axis_index("ra_2")

    def from_low(g):
        return jnp.where(ra_odd == 0, from_b_ref[g], from_a_ref[g])

    def from_high(g):
        return jnp.where(ra_odd == 0, from_a_ref[g], from_b_ref[g])

    return from_low, from_high


def chi_kernel(
    design_ref, observed_ref, weight_ref, code_ref,
    chi_ref, halo_ref, lines_ref, from_a_ref, from_b_ref, send_ref, win_ref,
):
    lane, row, half = grids()
    ra = lax.axis_index(RA)
    dec = lax.axis_index(DEC)
    from_low, from_high = ra_sides(from_a_ref, from_b_ref)
    for p in range(5):
        g, i = divmod(p, 4)
        value = jnp.where(row == 0, subs(from_low(g), -i), subs(from_high(g), 3 - i))
        found = columns_around(value, jnp.zeros(BLOCK, jnp.float32), p, lane, half)
        for b in range(3):
            win_ref[b, p] = found[b]

    halo = halo_ref[...]
    halo = jnp.where(row == 3, subs(halo, 3), subs(halo, 5))
    corner = [jnp.where(row == 3, from_low(2 + i), from_high(2 + i)) for i in range(7)]
    resid = corner[5]
    for p in range(5):
        resid = resid - corner[p] * halo[:, p : p + 1]
    acc = chi_ref[...] + jnp.where((row == 0) | (row == 3), corner[6] * resid * resid, 0.0)

    wanted = [edge_code(b, row) for b in range(3)]
    wanted[0] = jnp.where((lane == 0) & (half == 0), -1, wanted[0])
    wanted[2] = jnp.where((lane == 127) & (half == 1), -1, wanted[2])

    def body(k, acc):
        code = code_ref[k]
        hits = [code == x for x in wanted]
        resid = observed_ref[k]
        for p in range(5):
            source = jnp.where(hits[1], win_ref[1, p], win_ref[0, p])
            source = jnp.where(hits[2], win_ref[2, p], source)
            resid = resid - design_ref[p, k] * source
        w = jnp.where(hits[0] | hits[1] | hits[2], weight_ref[k], 0.0)
        return acc + w * resid * resid

    chi = jnp.sum(lax.fori_loop(0, 80, body, acc, unroll=4))
    base = jnp.where(lane == NQ, chi, jnp.broadcast_to(lines_ref[6:7, :], BLOCK))
    for g in range(32):
        send_ref[pl.ds(8 * g, 8), :] = base

    for i in range(3):
        place = ((ra + (15 + i)) & 15) * 16 + dec

        @pl.when(dec > 0)
        def _(i=i, place=place):
            send_ref[pl.ds(place - 1, 1), :] = base[:1] + lines_ref[2 * i : 2 * i + 1, :]

        @pl.when(dec < 15)
        def _(i=i, place=place):
            send_ref[pl.ds(place + 1, 1), :] = base[:1] + lines_ref[2 * i + 1 : 2 * i + 2, :]


def cross_kernel(
    design_ref, observed_ref, weight_ref, code_ref, send_ref, to_a_ref, to_b_ref, acc_ref
):
    lane, row, half = grids()
    for i, code in enumerate((0, 1, 2, 6, 7, 8)):
        acc = accumulate(design_ref, observed_ref, weight_ref, code_ref, code)
        for q in range(NQ):
            acc_ref[i, q] = acc[q]
    values = []
    for q in range(NQ):
        leave = [
            jnp.where(row == 0, acc_ref[b, q], jnp.where(row == 3, acc_ref[3 + b, q], 0.0)) for b in range(3)
        ]
        values.append(shift_sum(*leave, lane, half))
    by_neighbour(to_a_ref, to_b_ref, *pack_rows(values, row))


def stay_kernel(
    design_ref, observed_ref, weight_ref, code_ref, cross_ref, total_ref, acc_ref
):
    lane, row, half = grids()
    for b in range(3):
        acc = accumulate(design_ref, observed_ref, weight_ref, code_ref, 3 + b)
        for q in range(NQ):
            acc_ref[b, q] = acc[q]
    for q in range(NQ):
        stay = []
        for b in range(3):
            back, same, ahead = cross_ref[b, q], acc_ref[b, q], cross_ref[3 + b, q]
            stay.append(
                same + jnp.where(row < 3, subs(back, 7), 0.0) + jnp.where(row > 0, subs(ahead, 1), 0.0)
            )
        total_ref[q] = shift_sum(*stay, lane, half)


def solve(rhs, normal):
    lower = [[None] * 5 for _ in range(5)]
    inverse = [None] * 5
    for first in range(5):
        for second in range(first + 1):
            running = normal[second][first]
            for inner in range(second):
                running = running - lower[first][inner] * lower[second][inner]
            if first == second:
                inverse[first] = 1.0 / jnp.sqrt(running)
            else:
                lower[first][second] = running * inverse[second]
    forward = []
    for first in range(5):
        running = rhs[first]
        for inner in range(first):
            running = running - lower[first][inner] * forward[inner]
        forward.append(running * inverse[first])
    answer = [None] * 5
    for first in range(4, -1, -1):
        running = forward[first]
        for inner in range(first + 1, 5):
            running = running - lower[inner][first] * answer[inner]
        answer[first] = running * inverse[first]
    return answer


def solve_kernel(params_ref, total_ref, from_a_ref, from_b_ref, got_ref, new_ref, chi_ref):
    lane, row, half = grids()
    ra = lax.axis_index(RA)
    dec = lax.axis_index(DEC)

    def column(step):
        line = jnp.zeros((1, 128), jnp.float32)
        for i in range(3):
            place = ((ra + (15 + i)) & 15) * 16 + dec + step
            place = jnp.minimum(jnp.maximum(place, 0), 255)
            line = line + got_ref[pl.ds(place, 1), :]
        line = jnp.broadcast_to(line, BLOCK)
        out = line
        for r in range(1, 4):
            out = jnp.where(row == r, lanes(line, -32 * r), out)
        return out

    from_low = column(-1)
    from_high = column(1)
    ra_low, ra_high = ra_sides(from_a_ref, from_b_ref)
    sums = []
    for q in range(NQ):
        g, i = divmod(q, 4)
        sums.append(
            total_ref[q]
            + jnp.where(row == 0, subs(ra_low(g), -i), 0.0)
            + jnp.where(row == 3, subs(ra_high(g), 3 - i), 0.0)
            + jnp.where((lane == 0) & (half == 0), lanes(from_low, -q), 0.0)
            + jnp.where((lane == 127) & (half == 1), lanes(from_high, 127 - q), 0.0)
        )
    normal = [[None] * 5 for _ in range(5)]
    for place, (p, q) in enumerate(PAIRS):
        normal[p][q] = sums[5 + place]
        normal[q][p] = sums[5 + place]
    params = [params_ref[p] for p in range(5)]
    rhs = []
    for p in range(5):
        running = sums[p]
        for q in range(5):
            running = running - normal[p][q] * params[q]
        rhs.append(running)
    for p in range(5):
        normal[p][p] = normal[p][p] + 1.0
    delta = solve(rhs, normal)
    for p in range(5):
        new_ref[p] = params[p] + delta[p]
    all_sums = got_ref[pl.ds(0, 8), :]
    for g in range(1, 32):
        all_sums = all_sums + got_ref[pl.ds(8 * g, 8), :]
    chi = jnp.sum(jnp.where(lane == NQ, all_sums, 0.0))
    count = jnp.sum(jnp.where(lane == NQ + 1, all_sums, 0.0))
    chi_ref[0, 0] = chi / count


def exchange(value, axes, pairs):
    both = [(i, j) for i, j in pairs] + [(j, i) for i, j in pairs]
    return lax.ppermute(value, axes, both)


def f32(*shape):
    return jax.ShapeDtypeStruct(shape, jnp.float32)


def call(kernel, outs, n_in, scratch=(), flops=1000, smem_last=False, mib=2):
    specs = [VM] * len(outs)
    if smem_last:
        specs[-1] = SM
    return pl.pallas_call(
        kernel,
        out_shape=tuple(outs),
        in_specs=[VM] * n_in,
        out_specs=tuple(specs),
        scratch_shapes=list(scratch),
        cost_estimate=pl.CostEstimate(flops=flops, bytes_accessed=100000, transcendentals=0),
        compiler_params=pltpu.CompilerParams(vmem_limit_bytes=mib << 20),
    )


def scratch(*shape):
    return pltpu.VMEM(shape + BLOCK, jnp.float32)


def device_step(design, observed, weight, params, offsets, counts):
    design, observed, weight, params, offsets, counts = (
        blocked(x) for x in (design, observed, weight, params, offsets, counts)
    )
    (edge,) = call(edge_kernel, [f32(*BLOCK)], 1, (), EDGE_FLOPS)(params)
    dec_b = exchange(edge, DEC, [(i, i + 1) for i in range(1, 15, 2)])
    ra_b_pairs = [(i, (i + 1) % 16) for i in range(1, 16, 2)]
    ra_a_pairs = [(i, i + 1) for i in range(0, 16, 2)]
    message = f32(9, *BLOCK)
    to_a, to_b, packed, codes, again = call(
        column_kernel,
        [message, message, f32(7, *BLOCK), jax.ShapeDtypeStruct(BLOCK, jnp.int32), f32(*BLOCK)],
        7, (), 10_000_000, mib=6,
    )(design, observed, weight, offsets, counts, params, edge)
    from_b = exchange(to_b, RA, ra_b_pairs)
    dec_a = exchange(again, DEC, [(i, i + 1) for i in range(0, 16, 2)])
    from_a = exchange(to_a, RA, ra_a_pairs)
    lines, chi, halo, code = call(
        inside_kernel,
        [f32(*BLOCK), f32(*BLOCK), f32(*BLOCK), jax.ShapeDtypeStruct((80,) + BLOCK, jnp.int32)],
        10, [scratch(9, 5)], 300_000_000, mib=6,
    )(design, observed, weight, offsets, counts, params, packed, codes, dec_a, dec_b)
    slots = (design, observed, weight, code)
    (send,) = call(chi_kernel, [f32(256, 128)], 9, [scratch(3, 5)], 5_000_000, mib=6)(
        *slots, chi, halo, lines, from_a, from_b
    )
    got = lax.all_to_all(send.reshape(256, 1, 128), ALL, 0, 0, tiled=True).reshape(256, 128)
    sums = f32(5, *BLOCK)
    sums_a, sums_b, cross = call(
        cross_kernel, [sums, sums, f32(6, NQ, *BLOCK)], 5, (), 1_000_000_000, mib=6
    )(*slots, send)
    sums_b = exchange(sums_b, RA, ra_b_pairs)
    sums_a = exchange(sums_a, RA, ra_a_pairs)
    (total,) = call(
        stay_kernel, [f32(NQ, *BLOCK)], 5, [scratch(3, NQ)], 1_000_000_000, mib=6
    )(*slots, cross)
    new, chi = call(solve_kernel, [f32(5, *BLOCK), f32(1, 1)], 5, (), 100000, True)(
        params, total, sums_a, sums_b, got
    )
    return unblocked(new), chi.reshape(())


def solution(mesh):
    finer = Mesh(mesh.devices.reshape(2, 4, 2, 8, 2), ALL)
    return jax.shard_map(
        device_step,
        mesh=finer,
        in_specs=(
            P(None, None, RA, DEC),
            P(None, RA, DEC),
            P(None, RA, DEC),
            P(None, RA, DEC),
            P(None, RA, DEC),
            P(RA, DEC),
        ),
        out_specs=(P(None, RA, DEC), P()),
        check_vma=False,
    )
```

```python
import jax
import jax.numpy as jnp
from jax import lax
from jax.experimental import pallas as pl
from jax.experimental.pallas import tpu as pltpu
from jax.sharding import Mesh
from jax.sharding import PartitionSpec as P

RA = ("ra_0", "ra_1", "ra_2")
DEC = ("dec_0", "dec_1")
ALL = RA + DEC

PAIRS = [(p, q) for p in range(5) for q in range(p, 5)]
NQ = 20
CROSS = (0, 1, 2, 6, 7, 8)
SEED_FLOPS = 20_000_000_000
VM = pl.BlockSpec(memory_space=pltpu.VMEM)
SM = pl.BlockSpec(memory_space=pltpu.SMEM)
BLOCK = (8, 128)


def blocked(x):
    lead = x.shape[:-2]
    x = x.reshape(lead + (4, 2, 128))
    x = jnp.swapaxes(x, -3, -2)
    return x.reshape(lead + BLOCK)


def unblocked(x):
    lead = x.shape[:-2]
    x = x.reshape(lead + (2, 4, 128))
    x = jnp.swapaxes(x, -3, -2)
    return x.reshape(lead + (4, 256))


def grids():
    lane = lax.broadcasted_iota(jnp.int32, BLOCK, 1)
    sub = lax.broadcasted_iota(jnp.int32, BLOCK, 0)
    return lane, sub & 3, sub >> 2


def lanes(x, by):
    by = by % 128
    return x if by == 0 else pltpu.roll(x, by, 1)


def subs(x, by):
    by = by % 8
    return x if by == 0 else pltpu.roll(x, by, 0)


def seed_kernel(out_ref):
    out_ref[...] = jnp.zeros(BLOCK, jnp.float32)


def shift_sum(minus, mid, plus, lane, half):
    down = lanes(minus, 127)
    down = jnp.where(lane == 127, jnp.where(half == 0, subs(down, 4), 0.0), down)
    up = lanes(plus, 1)
    up = jnp.where(lane == 0, jnp.where(half == 1, subs(up, 4), 0.0), up)
    return mid + down + up


def accumulate(design_ref, observed_ref, weight_ref, code_ref, wanted):
    def body(k, acc):
        w = jnp.where(code_ref[k] == wanted, weight_ref[k], 0.0)
        d = [design_ref[p, k] for p in range(5)]
        o = observed_ref[k]
        wd = [w * x for x in d]
        new = [wd[p] * o for p in range(5)] + [wd[p] * d[q] for p, q in PAIRS]
        return tuple(x + y for x, y in zip(acc, new))

    return lax.fori_loop(0, 80, body, (jnp.zeros(BLOCK, jnp.float32),) * NQ, unroll=4)


def edge_code(b, row):
    return jnp.where(row == 0, b, jnp.where(row == 3, 6 + b, -1))


def by_neighbour(to_a_ref, to_b_ref, low, high, start=0):
    ra_odd = lax.axis_index("ra_2")
    for g in range(len(low)):
        to_a_ref[start + g] = jnp.where(ra_odd == 0, high[g], low[g])
        to_b_ref[start + g] = jnp.where(ra_odd == 0, low[g], high[g])


def pack_rows(values, row):
    count = (len(values) + 3) // 4
    low = [jnp.zeros(BLOCK, jnp.float32) for _ in range(count)]
    high = [jnp.zeros(BLOCK, jnp.float32) for _ in range(count)]
    for q, value in enumerate(values):
        g, i = divmod(q, 4)
        low[g] = jnp.where(row == i, subs(value, i), low[g])
        high[g] = jnp.where(row == i, subs(value, i - 3), high[g])
    return low, high


def column_kernel(
    design_ref, observed_ref, weight_ref, offsets_ref, counts_ref, params_ref, seed_ref,
    to_a_ref, to_b_ref, packed_ref, codes_ref,
):
    lane, row, half = grids()
    packed = [seed_ref[...]] * 7
    codes = jnp.full(BLOCK, 9, jnp.int32)
    counts = jnp.zeros(BLOCK, jnp.int32)
    for k in range(80):
        here = lane == jnp.where(half == 0, k, (k + 127) % 128)
        values = [design_ref[p, k] for p in range(5)] + [observed_ref[k], weight_ref[k]]
        packed = [jnp.where(here, lanes(x, k), y) for x, y in zip(values, packed)]
        codes = jnp.where(here, lanes(offsets_ref[k], k), codes)
    counts = counts_ref[...]
    counts = jnp.where(half == 0, counts[:, :1], counts[:, 127:])
    slot = jnp.where(half == 0, lane, (lane + 1) & 127)
    codes = jnp.where(counts > slot, codes, 9)
    for i in range(7):
        packed_ref[i] = packed[i]
    codes_ref[...] = codes
    corner = edge_code(2 * half, row)
    outside = packed[:6] + [jnp.where(codes == corner, packed[6], 0.0)]
    low, high = pack_rows([params_ref[p] for p in range(5)], row)
    by_neighbour(to_a_ref, to_b_ref, low + outside, high + outside)


def flatten(x, row, half):
    flat = x
    for r in range(1, 4):
        flat = jnp.where(row == r, lanes(x, 32 * r), flat)
    return [jnp.sum(jnp.where(half == j, flat, 0.0), axis=0, keepdims=True) for j in range(2)]


def columns_around(x, lane):
    below = lanes(x, 1)
    below = jnp.where(lane == 0, subs(below, 4), below)
    above = lanes(x, 127)
    above = jnp.where(lane == 127, subs(above, 4), above)
    return below, x, above


def lines_kernel(
    design_ref, observed_ref, weight_ref, offsets_ref, counts_ref, params_ref, packed_ref, codes_ref,
    lines_ref, code_ref, chi_ref, win_ref,
):
    lane, row, half = grids()
    counts = counts_ref[...]

    def mark(k, carry):
        code_ref[k] = jnp.where(counts > k, offsets_ref[k], 9)
        return carry

    lax.fori_loop(0, 80, mark, 0, unroll=8)
    zero = jnp.zeros(BLOCK, jnp.float32)
    d, o, weight, codes = [packed_ref[p] for p in range(5)], packed_ref[5], packed_ref[6], codes_ref[...]
    found = []
    for a in range(3):
        w = jnp.where(codes == 3 * a + 2 * half, weight, 0.0)
        wd = [w * x for x in d]
        terms = [wd[p] * o for p in range(5)] + [wd[p] * d[q] for p, q in PAIRS]
        out = zero
        for q in range(NQ):
            out = jnp.where(lane == q, jnp.sum(terms[q], axis=1, keepdims=True), out)
        found.append(out)
    back, same, ahead = found
    mid = same + jnp.where(row < 3, subs(back, 7), 0.0) + jnp.where(row > 0, subs(ahead, 1), 0.0)
    low = jnp.where(row == 3, subs(back, 3), 0.0)
    high = jnp.where(row == 0, subs(ahead, 5), 0.0)
    lines_ref[...] = jnp.zeros(BLOCK, jnp.float32)
    for i, x in enumerate((low, mid, high)):
        for j, line in enumerate(flatten(x, row, half)):
            lines_ref[2 * i + j : 2 * i + j + 1, :] = line
    lines_ref[6:7, :] = jnp.where(lane[:1] == NQ + 1, jnp.sum(counts.astype(jnp.float32)), 0.0)


    for p in range(5):
        value = params_ref[p]
        for a in range(3):
            found = columns_around(subs(value, (1, 0, 7)[a]), lane)
            for b in range(3):
                win_ref[3 * a + b, p] = found[b]
    inside = []
    for code in range(9):
        a, b = divmod(code, 3)
        off = (row == 0) if a == 0 else (row == 3) if a == 2 else (row < 0)
        if b == 0:
            off = off | ((lane == 0) & (half == 0))
        if b == 2:
            off = off | ((lane == 127) & (half == 1))
        inside.append(jnp.where(off, -1, code))

    def body(k, acc):
        code = code_ref[k]
        hits = [code == x for x in inside]
        resid = observed_ref[k]
        for p in range(5):
            source = win_ref[0, p]
            for c in range(1, 9):
                source = jnp.where(hits[c], win_ref[c, p], source)
            resid = resid - design_ref[p, k] * source
        some = hits[0]
        for c in range(1, 9):
            some = some | hits[c]
        w = jnp.where(some, weight_ref[k], 0.0)
        return acc + w * resid * resid

    chi_ref[...] = lax.fori_loop(0, 80, body, jnp.zeros(BLOCK, jnp.float32), unroll=4)


def ra_sides(from_a_ref, from_b_ref):
    ra_odd = lax.axis_index("ra_2")

    def from_low(g):
        return jnp.where(ra_odd == 0, from_b_ref[g], from_a_ref[g])

    def from_high(g):
        return jnp.where(ra_odd == 0, from_a_ref[g], from_b_ref[g])

    return from_low, from_high


def chi_kernel(
    design_ref, observed_ref, weight_ref, code_ref,
    chi_ref, packed_ref, codes_ref, lines_ref, dec_a_ref, dec_b_ref, from_a_ref, from_b_ref,
    send_ref, after_ref, win_ref,
):
    lane, row, half = grids()
    ra = lax.axis_index(RA)
    dec = lax.axis_index(DEC)
    from_low, from_high = ra_sides(from_a_ref, from_b_ref)
    for p in range(5):
        g, i = divmod(p, 4)
        value = jnp.where(row == 0, subs(from_low(g), -i), subs(from_high(g), 3 - i))
        found = columns_around(value, lane)
        for b in range(3):
            win_ref[b, p] = found[b]

    dec_odd = lax.axis_index("dec_1")
    halo = []
    for p in range(5):
        below = subs(jnp.where(dec_odd == 0, dec_b_ref[p], dec_a_ref[p]), 4)
        above = subs(jnp.where(dec_odd == 0, dec_a_ref[p], dec_b_ref[p]), 4)
        halo.append(jnp.where(half == 0, below[:, 127:], above[:, :1]))
    codes = codes_ref[...]
    acc = chi_ref[...]
    for a, shift, there in ((0, 1, row > 0), (1, 0, row >= 0), (2, 7, row < 3)):
        resid = packed_ref[5]
        for p in range(5):
            resid = resid - packed_ref[p] * subs(halo[p], shift)
        w = jnp.where((codes == 3 * a + 2 * half) & there, packed_ref[6], 0.0)
        acc = acc + w * resid * resid
    corner = [jnp.where(row == 3, from_low(2 + i), from_high(2 + i)) for i in range(7)]
    resid = corner[5]
    for p in range(5):
        resid = resid - corner[p] * jnp.where(row == 3, subs(halo[p], 3), subs(halo[p], 5))
    acc = acc + jnp.where((row == 0) | (row == 3), corner[6] * resid * resid, 0.0)

    wanted = [edge_code(b, row) for b in range(3)]
    wanted[0] = jnp.where((lane == 0) & (half == 0), -1, wanted[0])
    wanted[2] = jnp.where((lane == 127) & (half == 1), -1, wanted[2])

    def body(k, acc):
        code = code_ref[k]
        hits = [code == x for x in wanted]
        resid = observed_ref[k]
        for p in range(5):
            source = jnp.where(hits[1], win_ref[1, p], win_ref[0, p])
            source = jnp.where(hits[2], win_ref[2, p], source)
            resid = resid - design_ref[p, k] * source
        w = jnp.where(hits[0] | hits[1] | hits[2], weight_ref[k], 0.0)
        return acc + w * resid * resid

    chi = jnp.sum(lax.fori_loop(0, 80, body, acc, unroll=4))
    base = jnp.where(lane == NQ, chi, jnp.broadcast_to(lines_ref[6:7, :], BLOCK))
    after_ref[...] = base
    for g in range(32):
        send_ref[pl.ds(8 * g, 8), :] = base

    for i in range(3):
        place = ((ra + (15 + i)) & 15) * 16 + dec

        @pl.when(dec > 0)
        def _(i=i, place=place):
            send_ref[pl.ds(place - 1, 1), :] = base[:1] + lines_ref[2 * i : 2 * i + 1, :]

        @pl.when(dec < 15)
        def _(i=i, place=place):
            send_ref[pl.ds(place + 1, 1), :] = base[:1] + lines_ref[2 * i + 1 : 2 * i + 2, :]


def cross_kernel(
    design_ref, observed_ref, weight_ref, code_ref, after_ref, to_a_ref, to_b_ref, acc_ref
):
    lane, row, half = grids()
    for i, code in enumerate(CROSS):
        acc = accumulate(design_ref, observed_ref, weight_ref, code_ref, code)
        for q in range(NQ):
            acc_ref[i, q] = acc[q]
    values = []
    for q in range(NQ):
        leave = [
            jnp.where(row == 0, acc_ref[b, q], jnp.where(row == 3, acc_ref[3 + b, q], 0.0)) for b in range(3)
        ]
        values.append(shift_sum(*leave, lane, half))
    by_neighbour(to_a_ref, to_b_ref, *pack_rows(values, row))


def stay_kernel(
    design_ref, observed_ref, weight_ref, code_ref, cross_ref, total_ref, acc_ref
):
    lane, row, half = grids()
    for b in range(3):
        acc = accumulate(design_ref, observed_ref, weight_ref, code_ref, 3 + b)
        for q in range(NQ):
            acc_ref[b, q] = acc[q]
    for q in range(NQ):
        stay = []
        for b in range(3):
            back, same, ahead = cross_ref[b, q], acc_ref[b, q], cross_ref[3 + b, q]
            stay.append(
                same + jnp.where(row < 3, subs(back, 7), 0.0) + jnp.where(row > 0, subs(ahead, 1), 0.0)
            )
        total_ref[q] = shift_sum(*stay, lane, half)


def solve(rhs, normal):
    lower = [[None] * 5 for _ in range(5)]
    inverse = [None] * 5
    for first in range(5):
        for second in range(first + 1):
            running = normal[second][first]
            for inner in range(second):
                running = running - lower[first][inner] * lower[second][inner]
            if first == second:
                inverse[first] = 1.0 / jnp.sqrt(running)
            else:
                lower[first][second] = running * inverse[second]
    forward = []
    for first in range(5):
        running = rhs[first]
        for inner in range(first):
            running = running - lower[first][inner] * forward[inner]
        forward.append(running * inverse[first])
    answer = [None] * 5
    for first in range(4, -1, -1):
        running = forward[first]
        for inner in range(first + 1, 5):
            running = running - lower[inner][first] * answer[inner]
        answer[first] = running * inverse[first]
    return answer


def solve_kernel(params_ref, total_ref, from_a_ref, from_b_ref, got_ref, new_ref, chi_ref):
    lane, row, half = grids()
    ra = lax.axis_index(RA)
    dec = lax.axis_index(DEC)

    def column(step):
        line = jnp.zeros((1, 128), jnp.float32)
        for i in range(3):
            place = ((ra + (15 + i)) & 15) * 16 + dec + step
            place = jnp.minimum(jnp.maximum(place, 0), 255)
            line = line + got_ref[pl.ds(place, 1), :]
        line = jnp.broadcast_to(line, BLOCK)
        out = line
        for r in range(1, 4):
            out = jnp.where(row == r, lanes(line, -32 * r), out)
        return out

    from_low = column(-1)
    from_high = column(1)
    ra_low, ra_high = ra_sides(from_a_ref, from_b_ref)
    sums = []
    for q in range(NQ):
        g, i = divmod(q, 4)
        sums.append(
            total_ref[q]
            + jnp.where(row == 0, subs(ra_low(g), -i), 0.0)
            + jnp.where(row == 3, subs(ra_high(g), 3 - i), 0.0)
            + jnp.where((lane == 0) & (half == 0), lanes(from_low, -q), 0.0)
            + jnp.where((lane == 127) & (half == 1), lanes(from_high, 127 - q), 0.0)
        )
    normal = [[None] * 5 for _ in range(5)]
    for place, (p, q) in enumerate(PAIRS):
        normal[p][q] = sums[5 + place]
        normal[q][p] = sums[5 + place]
    params = [params_ref[p] for p in range(5)]
    rhs = []
    for p in range(5):
        running = sums[p]
        for q in range(5):
            running = running - normal[p][q] * params[q]
        rhs.append(running)
    for p in range(5):
        normal[p][p] = normal[p][p] + 1.0
    delta = solve(rhs, normal)
    for p in range(5):
        new_ref[p] = params[p] + delta[p]
    all_sums = got_ref[pl.ds(0, 8), :]
    for g in range(1, 32):
        all_sums = all_sums + got_ref[pl.ds(8 * g, 8), :]
    chi = jnp.sum(jnp.where(lane == NQ, all_sums, 0.0))
    count = jnp.sum(jnp.where(lane == NQ + 1, all_sums, 0.0))
    chi_ref[0, 0] = chi / count


def exchange(value, axes, pairs):
    both = [(i, j) for i, j in pairs] + [(j, i) for i, j in pairs]
    return lax.ppermute(value, axes, both)


def f32(*shape):
    return jax.ShapeDtypeStruct(shape, jnp.float32)


def call(kernel, outs, n_in, scratch=(), flops=1000, smem_last=False, mib=2):
    specs = [VM] * len(outs)
    if smem_last:
        specs[-1] = SM
    return pl.pallas_call(
        kernel,
        out_shape=tuple(outs),
        in_specs=[VM] * n_in,
        out_specs=tuple(specs),
        scratch_shapes=list(scratch),
        cost_estimate=pl.CostEstimate(flops=flops, bytes_accessed=100000, transcendentals=0),
        compiler_params=pltpu.CompilerParams(vmem_limit_bytes=mib << 20),
    )


def scratch(*shape):
    return pltpu.VMEM(shape + BLOCK, jnp.float32)


def device_step(design, observed, weight, params, offsets, counts):
    design, observed, weight, params, offsets, counts = (
        blocked(x) for x in (design, observed, weight, params, offsets, counts)
    )
    dec_b = exchange(params, DEC, [(i, i + 1) for i in range(1, 15, 2)])
    dec_a = exchange(params, DEC, [(i, i + 1) for i in range(0, 16, 2)])
    (seed,) = call(seed_kernel, [f32(*BLOCK)], 0, (), SEED_FLOPS)()
    ra_b_pairs = [(i, (i + 1) % 16) for i in range(1, 16, 2)]
    ra_a_pairs = [(i, i + 1) for i in range(0, 16, 2)]
    message = f32(9, *BLOCK)
    to_a, to_b, packed, codes = call(
        column_kernel,
        [message, message, f32(7, *BLOCK), jax.ShapeDtypeStruct(BLOCK, jnp.int32)],
        7, (), 10_000_000, mib=6,
    )(design, observed, weight, offsets, counts, params, seed)
    from_b = exchange(to_b, RA, ra_b_pairs)
    from_a = exchange(to_a, RA, ra_a_pairs)
    lines, code, chi = call(
        lines_kernel,
        [f32(*BLOCK), jax.ShapeDtypeStruct((80,) + BLOCK, jnp.int32), f32(*BLOCK)],
        8, [scratch(9, 5)], 300_000_000, mib=6,
    )(design, observed, weight, offsets, counts, params, packed, codes)
    slots = (design, observed, weight, code)
    send, after = call(
        chi_kernel, [f32(256, 128), f32(*BLOCK)], 12, [scratch(3, 5)], 5_000_000, mib=6
    )(*slots, chi, packed, codes, lines, dec_a, dec_b, from_a, from_b)
    got = lax.all_to_all(send.reshape(256, 1, 128), ALL, 0, 0, tiled=True).reshape(256, 128)
    sums = f32(5, *BLOCK)
    sums_a, sums_b, cross = call(
        cross_kernel, [sums, sums, f32(6, NQ, *BLOCK)], 5, (), 1_000_000_000, mib=6
    )(*slots, after)
    sums_b = exchange(sums_b, RA, ra_b_pairs)
    sums_a = exchange(sums_a, RA, ra_a_pairs)
    (total,) = call(
        stay_kernel, [f32(NQ, *BLOCK)], 5, [scratch(3, NQ)], 1_000_000_000, mib=6
    )(*slots, cross)
    new, chi = call(solve_kernel, [f32(5, *BLOCK), f32(1, 1)], 5, (), 100000, True)(
        params, total, sums_a, sums_b, got
    )
    return unblocked(new), chi.reshape(())


def solution(mesh):
    finer = Mesh(mesh.devices.reshape(2, 4, 2, 8, 2), ALL)
    return jax.shard_map(
        device_step,
        mesh=finer,
        in_specs=(
            P(None, None, RA, DEC),
            P(None, RA, DEC),
            P(None, RA, DEC),
            P(None, RA, DEC),
            P(None, RA, DEC),
            P(RA, DEC),
        ),
        out_specs=(P(None, RA, DEC), P()),
        check_vma=False,
    )
```

```python
import jax
import jax.numpy as jnp
from jax import lax
from jax.experimental import pallas as pl
from jax.experimental.pallas import tpu as pltpu
from jax.sharding import Mesh
from jax.sharding import PartitionSpec as P

RA = ("ra_0", "ra_1", "ra_2")
DEC = ("dec_0", "dec_1")
ALL = RA + DEC

PAIRS = [(p, q) for p in range(5) for q in range(p, 5)]
NQ = 20
CROSS = (0, 1, 2, 6, 7, 8)
SEED_FLOPS = 20_000_000_000
VM = pl.BlockSpec(memory_space=pltpu.VMEM)
SM = pl.BlockSpec(memory_space=pltpu.SMEM)
BLOCK = (8, 128)


def blocked(x):
    lead = x.shape[:-2]
    x = x.reshape(lead + (4, 2, 128))
    x = jnp.swapaxes(x, -3, -2)
    return x.reshape(lead + BLOCK)


def unblocked(x):
    lead = x.shape[:-2]
    x = x.reshape(lead + (2, 4, 128))
    x = jnp.swapaxes(x, -3, -2)
    return x.reshape(lead + (4, 256))


def grids():
    lane = lax.broadcasted_iota(jnp.int32, BLOCK, 1)
    sub = lax.broadcasted_iota(jnp.int32, BLOCK, 0)
    return lane, sub & 3, sub >> 2


def lanes(x, by):
    by = by % 128
    return x if by == 0 else pltpu.roll(x, by, 1)


def subs(x, by):
    by = by % 8
    return x if by == 0 else pltpu.roll(x, by, 0)


def seed_kernel(out_ref):
    out_ref[...] = jnp.zeros(BLOCK, jnp.float32)


def shift_sum(minus, mid, plus, lane, half):
    down = lanes(minus, 127)
    down = jnp.where(lane == 127, jnp.where(half == 0, subs(down, 4), 0.0), down)
    up = lanes(plus, 1)
    up = jnp.where(lane == 0, jnp.where(half == 1, subs(up, 4), 0.0), up)
    return mid + down + up


def accumulate(design_ref, observed_ref, weight_ref, code_ref, wanted):
    def body(k, acc):
        w = jnp.where(code_ref[k] == wanted, weight_ref[k], 0.0)
        d = [design_ref[p, k] for p in range(5)]
        o = observed_ref[k]
        wd = [w * x for x in d]
        new = [wd[p] * o for p in range(5)] + [wd[p] * d[q] for p, q in PAIRS]
        return tuple(x + y for x, y in zip(acc, new))

    return lax.fori_loop(0, 80, body, (jnp.zeros(BLOCK, jnp.float32),) * NQ, unroll=4)


def edge_code(b, row):
    return jnp.where(row == 0, b, jnp.where(row == 3, 6 + b, -1))


def by_neighbour(to_a_ref, to_b_ref, low, high, start=0):
    ra_odd = lax.axis_index("ra_2")
    for g in range(len(low)):
        to_a_ref[start + g] = jnp.where(ra_odd == 0, high[g], low[g])
        to_b_ref[start + g] = jnp.where(ra_odd == 0, low[g], high[g])


def pack_rows(values, row):
    count = (len(values) + 3) // 4
    low = [jnp.zeros(BLOCK, jnp.float32) for _ in range(count)]
    high = [jnp.zeros(BLOCK, jnp.float32) for _ in range(count)]
    for q, value in enumerate(values):
        g, i = divmod(q, 4)
        low[g] = jnp.where(row == i, subs(value, i), low[g])
        high[g] = jnp.where(row == i, subs(value, i - 3), high[g])
    return low, high


def column_kernel(
    design_ref, observed_ref, weight_ref, offsets_ref, counts_ref, params_ref, seed_ref,
    to_a_ref, to_b_ref, packed_ref, codes_ref,
):
    lane, row, half = grids()
    packed = [seed_ref[...]] * 7
    codes = jnp.full(BLOCK, 9, jnp.int32)
    counts = jnp.zeros(BLOCK, jnp.int32)
    for k in range(80):
        here = lane == jnp.where(half == 0, k, (k + 127) % 128)
        values = [design_ref[p, k] for p in range(5)] + [observed_ref[k], weight_ref[k]]
        packed = [jnp.where(here, lanes(x, k), y) for x, y in zip(values, packed)]
        codes = jnp.where(here, lanes(offsets_ref[k], k), codes)
    counts = counts_ref[...]
    counts = jnp.where(half == 0, counts[:, :1], counts[:, 127:])
    slot = jnp.where(half == 0, lane, (lane + 1) & 127)
    codes = jnp.where(counts > slot, codes, 9)
    for i in range(7):
        packed_ref[i] = packed[i]
    codes_ref[...] = codes
    corner = jnp.where(codes == edge_code(2 * half, row), packed[6], 0.0)
    values = [params_ref[p] for p in range(5)] + packed[:6] + [corner]
    by_neighbour(to_a_ref, to_b_ref, *pack_rows(values, row))


def flatten(x, row, half):
    flat = x
    for r in range(1, 4):
        flat = jnp.where(row == r, lanes(x, 32 * r), flat)
    return [jnp.sum(jnp.where(half == j, flat, 0.0), axis=0, keepdims=True) for j in range(2)]


def columns_around(x, lane):
    below = lanes(x, 1)
    below = jnp.where(lane == 0, subs(below, 4), below)
    above = lanes(x, 127)
    above = jnp.where(lane == 127, subs(above, 4), above)
    return below, x, above


def lines_kernel(
    design_ref, observed_ref, weight_ref, offsets_ref, counts_ref, params_ref, packed_ref, codes_ref,
    lines_ref, code_ref, chi_ref, win_ref,
):
    lane, row, half = grids()
    counts = counts_ref[...]

    def mark(k, carry):
        code_ref[k] = jnp.where(counts > k, offsets_ref[k], 9)
        return carry

    lax.fori_loop(0, 80, mark, 0, unroll=8)
    zero = jnp.zeros(BLOCK, jnp.float32)
    d, o, weight, codes = [packed_ref[p] for p in range(5)], packed_ref[5], packed_ref[6], codes_ref[...]
    found = []
    for a in range(3):
        w = jnp.where(codes == 3 * a + 2 * half, weight, 0.0)
        wd = [w * x for x in d]
        terms = [wd[p] * o for p in range(5)] + [wd[p] * d[q] for p, q in PAIRS]
        out = zero
        for q in range(NQ):
            out = jnp.where(lane == q, jnp.sum(terms[q], axis=1, keepdims=True), out)
        found.append(out)
    back, same, ahead = found
    mid = same + jnp.where(row < 3, subs(back, 7), 0.0) + jnp.where(row > 0, subs(ahead, 1), 0.0)
    low = jnp.where(row == 3, subs(back, 3), 0.0)
    high = jnp.where(row == 0, subs(ahead, 5), 0.0)
    lines_ref[...] = jnp.zeros(BLOCK, jnp.float32)
    for i, x in enumerate((low, mid, high)):
        for j, line in enumerate(flatten(x, row, half)):
            lines_ref[2 * i + j : 2 * i + j + 1, :] = line
    lines_ref[6:7, :] = jnp.where(lane[:1] == NQ + 1, jnp.sum(counts.astype(jnp.float32)), 0.0)


    for p in range(5):
        value = params_ref[p]
        for a in range(3):
            found = columns_around(subs(value, (1, 0, 7)[a]), lane)
            for b in range(3):
                win_ref[3 * a + b, p] = found[b]
    inside = []
    for code in range(9):
        a, b = divmod(code, 3)
        off = (row == 0) if a == 0 else (row == 3) if a == 2 else (row < 0)
        if b == 0:
            off = off | ((lane == 0) & (half == 0))
        if b == 2:
            off = off | ((lane == 127) & (half == 1))
        inside.append(jnp.where(off, -1, code))

    def body(k, acc):
        code = code_ref[k]
        hits = [code == x for x in inside]
        resid = observed_ref[k]
        for p in range(5):
            source = win_ref[0, p]
            for c in range(1, 9):
                source = jnp.where(hits[c], win_ref[c, p], source)
            resid = resid - design_ref[p, k] * source
        some = hits[0]
        for c in range(1, 9):
            some = some | hits[c]
        w = jnp.where(some, weight_ref[k], 0.0)
        return acc + w * resid * resid

    chi_ref[...] = lax.fori_loop(0, 80, body, jnp.zeros(BLOCK, jnp.float32), unroll=4)


def ra_sides(from_a_ref, from_b_ref):
    ra_odd = lax.axis_index("ra_2")

    def from_low(g):
        return jnp.where(ra_odd == 0, from_b_ref[g], from_a_ref[g])

    def from_high(g):
        return jnp.where(ra_odd == 0, from_a_ref[g], from_b_ref[g])

    return from_low, from_high


def chi_kernel(
    design_ref, observed_ref, weight_ref, code_ref,
    chi_ref, packed_ref, codes_ref, lines_ref, dec_a_ref, dec_b_ref, from_a_ref, from_b_ref,
    send_ref, after_ref, win_ref,
):
    lane, row, half = grids()
    ra = lax.axis_index(RA)
    dec = lax.axis_index(DEC)
    from_low, from_high = ra_sides(from_a_ref, from_b_ref)
    values = []
    for q in range(12):
        g, i = divmod(q, 4)
        values.append(jnp.where(row == 0, subs(from_low(g), -i), subs(from_high(g), 3 - i)))
    for p in range(5):
        found = columns_around(values[p], lane)
        for b in range(3):
            win_ref[b, p] = found[b]

    dec_odd = lax.axis_index("dec_1")
    halo = []
    for p in range(5):
        below = subs(jnp.where(dec_odd == 0, dec_b_ref[p], dec_a_ref[p]), 4)
        above = subs(jnp.where(dec_odd == 0, dec_a_ref[p], dec_b_ref[p]), 4)
        halo.append(jnp.where(half == 0, below[:, 127:], above[:, :1]))
    codes = codes_ref[...]
    acc = chi_ref[...]
    for a, shift, there in ((0, 1, row > 0), (1, 0, row >= 0), (2, 7, row < 3)):
        resid = packed_ref[5]
        for p in range(5):
            resid = resid - packed_ref[p] * subs(halo[p], shift)
        w = jnp.where((codes == 3 * a + 2 * half) & there, packed_ref[6], 0.0)
        acc = acc + w * resid * resid
    resid = values[10]
    for p in range(5):
        resid = resid - values[5 + p] * halo[p]
    acc = acc + jnp.where((row == 0) | (row == 3), values[11] * resid * resid, 0.0)

    wanted = [edge_code(b, row) for b in range(3)]
    wanted[0] = jnp.where((lane == 0) & (half == 0), -1, wanted[0])
    wanted[2] = jnp.where((lane == 127) & (half == 1), -1, wanted[2])

    def body(k, acc):
        code = code_ref[k]
        hits = [code == x for x in wanted]
        resid = observed_ref[k]
        for p in range(5):
            source = jnp.where(hits[1], win_ref[1, p], win_ref[0, p])
            source = jnp.where(hits[2], win_ref[2, p], source)
            resid = resid - design_ref[p, k] * source
        w = jnp.where(hits[0] | hits[1] | hits[2], weight_ref[k], 0.0)
        return acc + w * resid * resid

    chi = jnp.sum(lax.fori_loop(0, 80, body, acc, unroll=4))
    base = jnp.where(lane == NQ, chi, jnp.broadcast_to(lines_ref[6:7, :], BLOCK))
    after_ref[...] = base
    for g in range(32):
        send_ref[pl.ds(8 * g, 8), :] = base

    for i in range(3):
        place = ((ra + (15 + i)) & 15) * 16 + dec

        @pl.when(dec > 0)
        def _(i=i, place=place):
            send_ref[pl.ds(place - 1, 1), :] = base[:1] + lines_ref[2 * i : 2 * i + 1, :]

        @pl.when(dec < 15)
        def _(i=i, place=place):
            send_ref[pl.ds(place + 1, 1), :] = base[:1] + lines_ref[2 * i + 1 : 2 * i + 2, :]


def cross_kernel(
    design_ref, observed_ref, weight_ref, code_ref, after_ref, to_a_ref, to_b_ref, acc_ref
):
    lane, row, half = grids()
    for i, code in enumerate(CROSS):
        acc = accumulate(design_ref, observed_ref, weight_ref, code_ref, code)
        for q in range(NQ):
            acc_ref[i, q] = acc[q]
    values = []
    for q in range(NQ):
        leave = [
            jnp.where(row == 0, acc_ref[b, q], jnp.where(row == 3, acc_ref[3 + b, q], 0.0)) for b in range(3)
        ]
        values.append(shift_sum(*leave, lane, half))
    by_neighbour(to_a_ref, to_b_ref, *pack_rows(values, row))


def stay_kernel(
    design_ref, observed_ref, weight_ref, code_ref, cross_ref, total_ref, acc_ref
):
    lane, row, half = grids()
    for b in range(3):
        acc = accumulate(design_ref, observed_ref, weight_ref, code_ref, 3 + b)
        for q in range(NQ):
            acc_ref[b, q] = acc[q]
    for q in range(NQ):
        stay = []
        for b in range(3):
            back, same, ahead = cross_ref[b, q], acc_ref[b, q], cross_ref[3 + b, q]
            stay.append(
                same + jnp.where(row < 3, subs(back, 7), 0.0) + jnp.where(row > 0, subs(ahead, 1), 0.0)
            )
        total_ref[q] = shift_sum(*stay, lane, half)


def solve(rhs, normal):
    lower = [[None] * 5 for _ in range(5)]
    inverse = [None] * 5
    for first in range(5):
        for second in range(first + 1):
            running = normal[second][first]
            for inner in range(second):
                running = running - lower[first][inner] * lower[second][inner]
            if first == second:
                inverse[first] = 1.0 / jnp.sqrt(running)
            else:
                lower[first][second] = running * inverse[second]
    forward = []
    for first in range(5):
        running = rhs[first]
        for inner in range(first):
            running = running - lower[first][inner] * forward[inner]
        forward.append(running * inverse[first])
    answer = [None] * 5
    for first in range(4, -1, -1):
        running = forward[first]
        for inner in range(first + 1, 5):
            running = running - lower[inner][first] * answer[inner]
        answer[first] = running * inverse[first]
    return answer


def solve_kernel(params_ref, total_ref, from_a_ref, from_b_ref, got_ref, new_ref, chi_ref):
    lane, row, half = grids()
    ra = lax.axis_index(RA)
    dec = lax.axis_index(DEC)

    def column(step):
        line = jnp.zeros((1, 128), jnp.float32)
        for i in range(3):
            place = ((ra + (15 + i)) & 15) * 16 + dec + step
            place = jnp.minimum(jnp.maximum(place, 0), 255)
            line = line + got_ref[pl.ds(place, 1), :]
        line = jnp.broadcast_to(line, BLOCK)
        out = line
        for r in range(1, 4):
            out = jnp.where(row == r, lanes(line, -32 * r), out)
        return out

    from_low = column(-1)
    from_high = column(1)
    ra_low, ra_high = ra_sides(from_a_ref, from_b_ref)
    sums = []
    for q in range(NQ):
        g, i = divmod(q, 4)
        sums.append(
            total_ref[q]
            + jnp.where(row == 0, subs(ra_low(g), -i), 0.0)
            + jnp.where(row == 3, subs(ra_high(g), 3 - i), 0.0)
            + jnp.where((lane == 0) & (half == 0), lanes(from_low, -q), 0.0)
            + jnp.where((lane == 127) & (half == 1), lanes(from_high, 127 - q), 0.0)
        )
    normal = [[None] * 5 for _ in range(5)]
    for place, (p, q) in enumerate(PAIRS):
        normal[p][q] = sums[5 + place]
        normal[q][p] = sums[5 + place]
    params = [params_ref[p] for p in range(5)]
    rhs = []
    for p in range(5):
        running = sums[p]
        for q in range(5):
            running = running - normal[p][q] * params[q]
        rhs.append(running)
    for p in range(5):
        normal[p][p] = normal[p][p] + 1.0
    delta = solve(rhs, normal)
    for p in range(5):
        new_ref[p] = params[p] + delta[p]
    all_sums = got_ref[pl.ds(0, 8), :]
    for g in range(1, 32):
        all_sums = all_sums + got_ref[pl.ds(8 * g, 8), :]
    chi = jnp.sum(jnp.where(lane == NQ, all_sums, 0.0))
    count = jnp.sum(jnp.where(lane == NQ + 1, all_sums, 0.0))
    chi_ref[0, 0] = chi / count


def exchange(value, axes, pairs):
    both = [(i, j) for i, j in pairs] + [(j, i) for i, j in pairs]
    return lax.ppermute(value, axes, both)


def f32(*shape):
    return jax.ShapeDtypeStruct(shape, jnp.float32)


def call(kernel, outs, n_in, scratch=(), flops=1000, smem_last=False, mib=2):
    specs = [VM] * len(outs)
    if smem_last:
        specs[-1] = SM
    return pl.pallas_call(
        kernel,
        out_shape=tuple(outs),
        in_specs=[VM] * n_in,
        out_specs=tuple(specs),
        scratch_shapes=list(scratch),
        cost_estimate=pl.CostEstimate(flops=flops, bytes_accessed=100000, transcendentals=0),
        compiler_params=pltpu.CompilerParams(vmem_limit_bytes=mib << 20),
    )


def scratch(*shape):
    return pltpu.VMEM(shape + BLOCK, jnp.float32)


def device_step(design, observed, weight, params, offsets, counts):
    design, observed, weight, params, offsets, counts = (
        blocked(x) for x in (design, observed, weight, params, offsets, counts)
    )
    dec_b = exchange(params, DEC, [(i, i + 1) for i in range(1, 15, 2)])
    dec_a = exchange(params, DEC, [(i, i + 1) for i in range(0, 16, 2)])
    (seed,) = call(seed_kernel, [f32(*BLOCK)], 0, (), SEED_FLOPS)()
    ra_b_pairs = [(i, (i + 1) % 16) for i in range(1, 16, 2)]
    ra_a_pairs = [(i, i + 1) for i in range(0, 16, 2)]
    message = f32(3, *BLOCK)
    to_a, to_b, packed, codes = call(
        column_kernel,
        [message, message, f32(7, *BLOCK), jax.ShapeDtypeStruct(BLOCK, jnp.int32)],
        7, (), 10_000_000, mib=6,
    )(design, observed, weight, offsets, counts, params, seed)
    from_b = exchange(to_b, RA, ra_b_pairs)
    from_a = exchange(to_a, RA, ra_a_pairs)
    lines, code, chi = call(
        lines_kernel,
        [f32(*BLOCK), jax.ShapeDtypeStruct((80,) + BLOCK, jnp.int32), f32(*BLOCK)],
        8, [scratch(9, 5)], 300_000_000, mib=6,
    )(design, observed, weight, offsets, counts, params, packed, codes)
    slots = (design, observed, weight, code)
    send, after = call(
        chi_kernel, [f32(256, 128), f32(*BLOCK)], 12, [scratch(3, 5)], 5_000_000, mib=6
    )(*slots, chi, packed, codes, lines, dec_a, dec_b, from_a, from_b)
    got = lax.all_to_all(send.reshape(256, 1, 128), ALL, 0, 0, tiled=True).reshape(256, 128)
    sums = f32(5, *BLOCK)
    sums_a, sums_b, cross = call(
        cross_kernel, [sums, sums, f32(6, NQ, *BLOCK)], 5, (), 1_000_000_000, mib=6
    )(*slots, after)
    sums_b = exchange(sums_b, RA, ra_b_pairs)
    sums_a = exchange(sums_a, RA, ra_a_pairs)
    (total,) = call(
        stay_kernel, [f32(NQ, *BLOCK)], 5, [scratch(3, NQ)], 1_000_000_000, mib=6
    )(*slots, cross)
    new, chi = call(solve_kernel, [f32(5, *BLOCK), f32(1, 1)], 5, (), 100000, True)(
        params, total, sums_a, sums_b, got
    )
    return unblocked(new), chi.reshape(())


def solution(mesh):
    finer = Mesh(mesh.devices.reshape(2, 4, 2, 8, 2), ALL)
    return jax.shard_map(
        device_step,
        mesh=finer,
        in_specs=(
            P(None, None, RA, DEC),
            P(None, RA, DEC),
            P(None, RA, DEC),
            P(None, RA, DEC),
            P(None, RA, DEC),
            P(RA, DEC),
        ),
        out_specs=(P(None, RA, DEC), P()),
        check_vma=False,
    )
```

```python
import jax
import jax.numpy as jnp
from jax import lax
from jax.experimental import pallas as pl
from jax.experimental.pallas import tpu as pltpu
from jax.sharding import Mesh
from jax.sharding import PartitionSpec as P

RA = ("ra_0", "ra_1", "ra_2")
DEC = ("dec_0", "dec_1")
ALL = RA + DEC

PAIRS = [(p, q) for p in range(5) for q in range(p, 5)]
NQ = 20
CROSS = (0, 1, 2, 6, 7, 8)
SEED_FLOPS = 20_000_000_000
VM = pl.BlockSpec(memory_space=pltpu.VMEM)
SM = pl.BlockSpec(memory_space=pltpu.SMEM)
BLOCK = (8, 128)


def blocked(x):
    lead = x.shape[:-2]
    x = x.reshape(lead + (4, 2, 128))
    x = jnp.swapaxes(x, -3, -2)
    return x.reshape(lead + BLOCK)


def unblocked(x):
    lead = x.shape[:-2]
    x = x.reshape(lead + (2, 4, 128))
    x = jnp.swapaxes(x, -3, -2)
    return x.reshape(lead + (4, 256))


def grids():
    lane = lax.broadcasted_iota(jnp.int32, BLOCK, 1)
    sub = lax.broadcasted_iota(jnp.int32, BLOCK, 0)
    return lane, sub & 3, sub >> 2


def lanes(x, by):
    by = by % 128
    return x if by == 0 else pltpu.roll(x, by, 1)


def subs(x, by):
    by = by % 8
    return x if by == 0 else pltpu.roll(x, by, 0)


def seed_kernel(out_ref):
    out_ref[...] = jnp.zeros(BLOCK, jnp.float32)


def shift_sum(minus, mid, plus, lane, half):
    down = lanes(minus, 127)
    down = jnp.where(lane == 127, jnp.where(half == 0, subs(down, 4), 0.0), down)
    up = lanes(plus, 1)
    up = jnp.where(lane == 0, jnp.where(half == 1, subs(up, 4), 0.0), up)
    return mid + down + up


def accumulate(design_ref, observed_ref, weight_ref, code_ref, wanted):
    def body(k, acc):
        w = jnp.where(code_ref[k] == wanted, weight_ref[k], 0.0)
        d = [design_ref[p, k] for p in range(5)]
        o = observed_ref[k]
        wd = [w * x for x in d]
        new = [wd[p] * o for p in range(5)] + [wd[p] * d[q] for p, q in PAIRS]
        return tuple(x + y for x, y in zip(acc, new))

    return lax.fori_loop(0, 80, body, (jnp.zeros(BLOCK, jnp.float32),) * NQ, unroll=4)


def edge_code(b, row):
    return jnp.where(row == 0, b, jnp.where(row == 3, 6 + b, -1))


def by_neighbour(to_a_ref, to_b_ref, low, high, start=0):
    ra_odd = lax.axis_index("ra_2")
    for g in range(len(low)):
        to_a_ref[start + g] = jnp.where(ra_odd == 0, high[g], low[g])
        to_b_ref[start + g] = jnp.where(ra_odd == 0, low[g], high[g])


def pack_rows(values, row):
    count = (len(values) + 3) // 4
    low = [jnp.zeros(BLOCK, jnp.float32) for _ in range(count)]
    high = [jnp.zeros(BLOCK, jnp.float32) for _ in range(count)]
    for q, value in enumerate(values):
        g, i = divmod(q, 4)
        low[g] = jnp.where(row == i, subs(value, i), low[g])
        high[g] = jnp.where(row == i, subs(value, i - 3), high[g])
    return low, high


def column_kernel(
    design_ref, observed_ref, weight_ref, offsets_ref, counts_ref, params_ref, seed_ref,
    to_a_ref, to_b_ref, packed_ref, codes_ref, again_ref,
):
    lane, row, half = grids()
    again_ref[...] = params_ref[...]
    packed = [seed_ref[...]] * 7
    codes = jnp.full(BLOCK, 9, jnp.int32)
    counts = jnp.zeros(BLOCK, jnp.int32)
    for k in range(80):
        here = lane == jnp.where(half == 0, k, (k + 127) % 128)
        values = [design_ref[p, k] for p in range(5)] + [observed_ref[k], weight_ref[k]]
        packed = [jnp.where(here, lanes(x, k), y) for x, y in zip(values, packed)]
        codes = jnp.where(here, lanes(offsets_ref[k], k), codes)
    counts = counts_ref[...]
    counts = jnp.where(half == 0, counts[:, :1], counts[:, 127:])
    slot = jnp.where(half == 0, lane, (lane + 1) & 127)
    codes = jnp.where(counts > slot, codes, 9)
    for i in range(7):
        packed_ref[i] = packed[i]
    codes_ref[...] = codes
    corner = jnp.where(codes == edge_code(2 * half, row), packed[6], 0.0)
    values = [params_ref[p] for p in range(5)] + packed[:6] + [corner]
    by_neighbour(to_a_ref, to_b_ref, *pack_rows(values, row))


def flatten(x, row, half):
    flat = x
    for r in range(1, 4):
        flat = jnp.where(row == r, lanes(x, 32 * r), flat)
    return [jnp.sum(jnp.where(half == j, flat, 0.0), axis=0, keepdims=True) for j in range(2)]


def columns_around(x, lane):
    below = lanes(x, 1)
    below = jnp.where(lane == 0, subs(below, 4), below)
    above = lanes(x, 127)
    above = jnp.where(lane == 127, subs(above, 4), above)
    return below, x, above


def lines_kernel(
    design_ref, observed_ref, weight_ref, offsets_ref, counts_ref, params_ref, packed_ref, codes_ref,
    lines_ref, code_ref, chi_ref, win_ref,
):
    lane, row, half = grids()
    counts = counts_ref[...]

    def mark(k, carry):
        code_ref[k] = jnp.where(counts > k, offsets_ref[k], 9)
        return carry

    lax.fori_loop(0, 80, mark, 0, unroll=8)
    zero = jnp.zeros(BLOCK, jnp.float32)
    d, o, weight, codes = [packed_ref[p] for p in range(5)], packed_ref[5], packed_ref[6], codes_ref[...]
    found = []
    for a in range(3):
        w = jnp.where(codes == 3 * a + 2 * half, weight, 0.0)
        wd = [w * x for x in d]
        terms = [wd[p] * o for p in range(5)] + [wd[p] * d[q] for p, q in PAIRS]
        out = zero
        for q in range(NQ):
            out = jnp.where(lane == q, jnp.sum(terms[q], axis=1, keepdims=True), out)
        found.append(out)
    back, same, ahead = found
    mid = same + jnp.where(row < 3, subs(back, 7), 0.0) + jnp.where(row > 0, subs(ahead, 1), 0.0)
    low = jnp.where(row == 3, subs(back, 3), 0.0)
    high = jnp.where(row == 0, subs(ahead, 5), 0.0)
    lines_ref[...] = jnp.zeros(BLOCK, jnp.float32)
    for i, x in enumerate((low, mid, high)):
        for j, line in enumerate(flatten(x, row, half)):
            lines_ref[2 * i + j : 2 * i + j + 1, :] = line
    lines_ref[6:7, :] = jnp.where(lane[:1] == NQ + 1, jnp.sum(counts.astype(jnp.float32)), 0.0)


    for p in range(5):
        value = params_ref[p]
        for a in range(3):
            found = columns_around(subs(value, (1, 0, 7)[a]), lane)
            for b in range(3):
                win_ref[3 * a + b, p] = found[b]
    inside = []
    for code in range(9):
        a, b = divmod(code, 3)
        off = (row == 0) if a == 0 else (row == 3) if a == 2 else (row < 0)
        if b == 0:
            off = off | ((lane == 0) & (half == 0))
        if b == 2:
            off = off | ((lane == 127) & (half == 1))
        inside.append(jnp.where(off, -1, code))

    def body(k, acc):
        code = code_ref[k]
        hits = [code == x for x in inside]
        resid = observed_ref[k]
        for p in range(5):
            source = win_ref[0, p]
            for c in range(1, 9):
                source = jnp.where(hits[c], win_ref[c, p], source)
            resid = resid - design_ref[p, k] * source
        some = hits[0]
        for c in range(1, 9):
            some = some | hits[c]
        w = jnp.where(some, weight_ref[k], 0.0)
        return acc + w * resid * resid

    chi_ref[...] = lax.fori_loop(0, 80, body, jnp.zeros(BLOCK, jnp.float32), unroll=4)


def ra_sides(from_a_ref, from_b_ref):
    ra_odd = lax.axis_index("ra_2")

    def from_low(g):
        return jnp.where(ra_odd == 0, from_b_ref[g], from_a_ref[g])

    def from_high(g):
        return jnp.where(ra_odd == 0, from_a_ref[g], from_b_ref[g])

    return from_low, from_high


def chi_kernel(
    design_ref, observed_ref, weight_ref, code_ref,
    chi_ref, packed_ref, codes_ref, lines_ref, dec_a_ref, dec_b_ref, from_a_ref, from_b_ref,
    send_ref, after_ref, win_ref,
):
    lane, row, half = grids()
    ra = lax.axis_index(RA)
    dec = lax.axis_index(DEC)
    from_low, from_high = ra_sides(from_a_ref, from_b_ref)
    values = []
    for q in range(12):
        g, i = divmod(q, 4)
        values.append(jnp.where(row == 0, subs(from_low(g), -i), subs(from_high(g), 3 - i)))
    for p in range(5):
        found = columns_around(values[p], lane)
        for b in range(3):
            win_ref[b, p] = found[b]

    dec_odd = lax.axis_index("dec_1")
    halo = []
    for p in range(5):
        below = subs(jnp.where(dec_odd == 0, dec_b_ref[p], dec_a_ref[p]), 4)
        above = subs(jnp.where(dec_odd == 0, dec_a_ref[p], dec_b_ref[p]), 4)
        halo.append(jnp.where(half == 0, below[:, 127:], above[:, :1]))
    codes = codes_ref[...]
    acc = chi_ref[...]
    for a, shift, there in ((0, 1, row > 0), (1, 0, row >= 0), (2, 7, row < 3)):
        resid = packed_ref[5]
        for p in range(5):
            resid = resid - packed_ref[p] * subs(halo[p], shift)
        w = jnp.where((codes == 3 * a + 2 * half) & there, packed_ref[6], 0.0)
        acc = acc + w * resid * resid
    resid = values[10]
    for p in range(5):
        resid = resid - values[5 + p] * halo[p]
    acc = acc + jnp.where((row == 0) | (row == 3), values[11] * resid * resid, 0.0)

    wanted = [edge_code(b, row) for b in range(3)]
    wanted[0] = jnp.where((lane == 0) & (half == 0), -1, wanted[0])
    wanted[2] = jnp.where((lane == 127) & (half == 1), -1, wanted[2])

    def body(k, acc):
        code = code_ref[k]
        hits = [code == x for x in wanted]
        resid = observed_ref[k]
        for p in range(5):
            source = jnp.where(hits[1], win_ref[1, p], win_ref[0, p])
            source = jnp.where(hits[2], win_ref[2, p], source)
            resid = resid - design_ref[p, k] * source
        w = jnp.where(hits[0] | hits[1] | hits[2], weight_ref[k], 0.0)
        return acc + w * resid * resid

    chi = jnp.sum(lax.fori_loop(0, 80, body, acc, unroll=4))
    base = jnp.where(lane == NQ, chi, jnp.broadcast_to(lines_ref[6:7, :], BLOCK))
    after_ref[...] = base
    for g in range(32):
        send_ref[pl.ds(8 * g, 8), :] = base

    for i in range(3):
        place = ((ra + (15 + i)) & 15) * 16 + dec

        @pl.when(dec > 0)
        def _(i=i, place=place):
            send_ref[pl.ds(place - 1, 1), :] = base[:1] + lines_ref[2 * i : 2 * i + 1, :]

        @pl.when(dec < 15)
        def _(i=i, place=place):
            send_ref[pl.ds(place + 1, 1), :] = base[:1] + lines_ref[2 * i + 1 : 2 * i + 2, :]


def cross_kernel(
    design_ref, observed_ref, weight_ref, code_ref, after_ref, to_a_ref, to_b_ref, acc_ref
):
    lane, row, half = grids()
    for i, code in enumerate(CROSS):
        acc = accumulate(design_ref, observed_ref, weight_ref, code_ref, code)
        for q in range(NQ):
            acc_ref[i, q] = acc[q]
    values = []
    for q in range(NQ):
        leave = [
            jnp.where(row == 0, acc_ref[b, q], jnp.where(row == 3, acc_ref[3 + b, q], 0.0)) for b in range(3)
        ]
        values.append(shift_sum(*leave, lane, half))
    by_neighbour(to_a_ref, to_b_ref, *pack_rows(values, row))


def stay_kernel(
    design_ref, observed_ref, weight_ref, code_ref, cross_ref, total_ref, acc_ref
):
    lane, row, half = grids()
    for b in range(3):
        acc = accumulate(design_ref, observed_ref, weight_ref, code_ref, 3 + b)
        for q in range(NQ):
            acc_ref[b, q] = acc[q]
    for q in range(NQ):
        stay = []
        for b in range(3):
            back, same, ahead = cross_ref[b, q], acc_ref[b, q], cross_ref[3 + b, q]
            stay.append(
                same + jnp.where(row < 3, subs(back, 7), 0.0) + jnp.where(row > 0, subs(ahead, 1), 0.0)
            )
        total_ref[q] = shift_sum(*stay, lane, half)


def solve(rhs, normal):
    lower = [[None] * 5 for _ in range(5)]
    inverse = [None] * 5
    for first in range(5):
        for second in range(first + 1):
            running = normal[second][first]
            for inner in range(second):
                running = running - lower[first][inner] * lower[second][inner]
            if first == second:
                inverse[first] = 1.0 / jnp.sqrt(running)
            else:
                lower[first][second] = running * inverse[second]
    forward = []
    for first in range(5):
        running = rhs[first]
        for inner in range(first):
            running = running - lower[first][inner] * forward[inner]
        forward.append(running * inverse[first])
    answer = [None] * 5
    for first in range(4, -1, -1):
        running = forward[first]
        for inner in range(first + 1, 5):
            running = running - lower[inner][first] * answer[inner]
        answer[first] = running * inverse[first]
    return answer


def solve_kernel(params_ref, total_ref, from_a_ref, from_b_ref, got_ref, new_ref, chi_ref):
    lane, row, half = grids()
    ra = lax.axis_index(RA)
    dec = lax.axis_index(DEC)

    def column(step):
        line = jnp.zeros((1, 128), jnp.float32)
        for i in range(3):
            place = ((ra + (15 + i)) & 15) * 16 + dec + step
            place = jnp.minimum(jnp.maximum(place, 0), 255)
            line = line + got_ref[pl.ds(place, 1), :]
        line = jnp.broadcast_to(line, BLOCK)
        out = line
        for r in range(1, 4):
            out = jnp.where(row == r, lanes(line, -32 * r), out)
        return out

    from_low = column(-1)
    from_high = column(1)
    ra_low, ra_high = ra_sides(from_a_ref, from_b_ref)
    sums = []
    for q in range(NQ):
        g, i = divmod(q, 4)
        sums.append(
            total_ref[q]
            + jnp.where(row == 0, subs(ra_low(g), -i), 0.0)
            + jnp.where(row == 3, subs(ra_high(g), 3 - i), 0.0)
            + jnp.where((lane == 0) & (half == 0), lanes(from_low, -q), 0.0)
            + jnp.where((lane == 127) & (half == 1), lanes(from_high, 127 - q), 0.0)
        )
    normal = [[None] * 5 for _ in range(5)]
    for place, (p, q) in enumerate(PAIRS):
        normal[p][q] = sums[5 + place]
        normal[q][p] = sums[5 + place]
    params = [params_ref[p] for p in range(5)]
    rhs = []
    for p in range(5):
        running = sums[p]
        for q in range(5):
            running = running - normal[p][q] * params[q]
        rhs.append(running)
    for p in range(5):
        normal[p][p] = normal[p][p] + 1.0
    delta = solve(rhs, normal)
    for p in range(5):
        new_ref[p] = params[p] + delta[p]
    all_sums = got_ref[pl.ds(0, 8), :]
    for g in range(1, 32):
        all_sums = all_sums + got_ref[pl.ds(8 * g, 8), :]
    chi = jnp.sum(jnp.where(lane == NQ, all_sums, 0.0))
    count = jnp.sum(jnp.where(lane == NQ + 1, all_sums, 0.0))
    chi_ref[0, 0] = chi / count


def exchange(value, axes, pairs):
    both = [(i, j) for i, j in pairs] + [(j, i) for i, j in pairs]
    return lax.ppermute(value, axes, both)


def f32(*shape):
    return jax.ShapeDtypeStruct(shape, jnp.float32)


def call(kernel, outs, n_in, scratch=(), flops=1000, smem_last=False, mib=2):
    specs = [VM] * len(outs)
    if smem_last:
        specs[-1] = SM
    return pl.pallas_call(
        kernel,
        out_shape=tuple(outs),
        in_specs=[VM] * n_in,
        out_specs=tuple(specs),
        scratch_shapes=list(scratch),
        cost_estimate=pl.CostEstimate(flops=flops, bytes_accessed=100000, transcendentals=0),
        compiler_params=pltpu.CompilerParams(vmem_limit_bytes=mib << 20),
    )


def scratch(*shape):
    return pltpu.VMEM(shape + BLOCK, jnp.float32)


def device_step(design, observed, weight, params, offsets, counts):
    design, observed, weight, params, offsets, counts = (
        blocked(x) for x in (design, observed, weight, params, offsets, counts)
    )
    dec_b = exchange(params, DEC, [(i, i + 1) for i in range(1, 15, 2)])
    (seed,) = call(seed_kernel, [f32(*BLOCK)], 0, (), SEED_FLOPS)()
    ra_b_pairs = [(i, (i + 1) % 16) for i in range(1, 16, 2)]
    ra_a_pairs = [(i, i + 1) for i in range(0, 16, 2)]
    message = f32(3, *BLOCK)
    to_a, to_b, packed, codes, again = call(
        column_kernel,
        [message, message, f32(7, *BLOCK), jax.ShapeDtypeStruct(BLOCK, jnp.int32),
         f32(5, *BLOCK)],
        7, (), 10_000_000, mib=6,
    )(design, observed, weight, offsets, counts, params, seed)
    dec_a = exchange(again, DEC, [(i, i + 1) for i in range(0, 16, 2)])
    from_b = exchange(to_b, RA, ra_b_pairs)
    from_a = exchange(to_a, RA, ra_a_pairs)
    lines, code, chi = call(
        lines_kernel,
        [f32(*BLOCK), jax.ShapeDtypeStruct((80,) + BLOCK, jnp.int32), f32(*BLOCK)],
        8, [scratch(9, 5)], 300_000_000, mib=6,
    )(design, observed, weight, offsets, counts, params, packed, codes)
    slots = (design, observed, weight, code)
    send, after = call(
        chi_kernel, [f32(256, 128), f32(*BLOCK)], 12, [scratch(3, 5)], 5_000_000, mib=6
    )(*slots, chi, packed, codes, lines, dec_a, dec_b, from_a, from_b)
    got = lax.all_to_all(send.reshape(256, 1, 128), ALL, 0, 0, tiled=True).reshape(256, 128)
    sums = f32(5, *BLOCK)
    sums_a, sums_b, cross = call(
        cross_kernel, [sums, sums, f32(6, NQ, *BLOCK)], 5, (), 1_000_000_000, mib=6
    )(*slots, after)
    sums_b = exchange(sums_b, RA, ra_b_pairs)
    sums_a = exchange(sums_a, RA, ra_a_pairs)
    (total,) = call(
        stay_kernel, [f32(NQ, *BLOCK)], 5, [scratch(3, NQ)], 1_000_000_000, mib=6
    )(*slots, cross)
    new, chi = call(solve_kernel, [f32(5, *BLOCK), f32(1, 1)], 5, (), 100000, True)(
        params, total, sums_a, sums_b, got
    )
    return unblocked(new), chi.reshape(())


def solution(mesh):
    finer = Mesh(mesh.devices.reshape(2, 4, 2, 8, 2), ALL)
    return jax.shard_map(
        device_step,
        mesh=finer,
        in_specs=(
            P(None, None, RA, DEC),
            P(None, RA, DEC),
            P(None, RA, DEC),
            P(None, RA, DEC),
            P(None, RA, DEC),
            P(RA, DEC),
        ),
        out_specs=(P(None, RA, DEC), P()),
        check_vma=False,
    )
```
